512 devices in a mesh: pipe: 16 (over y, core), tensor: 32 (over z, x).
Axes of the slice: x: 4, y: 8, z: 8, core: 2. Of those that a mesh axis runs over, the one named last changes fastest.
Arguments:
- patches: bfloat16 [262144, 1280], P(('pipe', 'tensor')), may hold values from -6 to 6
- attn_gain: float32 [1280], replicated, may hold values from 0.25 to 1.75
- w_qkv: bfloat16 [1280, 3840], P('tensor', 'pipe'), may hold values from -0.1118034 to 0.1118034
- w_out: bfloat16 [1280, 1280], P('tensor', 'pipe'), may hold values from -0.15625 to 0.15625
- merge_gain: float32 [1280], replicated, may hold values from 0.25 to 1.75
- window_ids: int32 [262144], P(('pipe', 'tensor')), may hold values from 0 to 127, as said below
- image_patches: int32 [2048], P(('pipe', 'tensor')), may hold values from 0 to 512, as said below
- image_sample: int32 [2048], P(('pipe', 'tensor')), may hold values from 0 to 7
Outputs:
- vision_seq: bfloat16 [16, 128, 32, 5120], P('pipe', None, 'tensor')
The draws below stay inside these ranges and needn't reach their ends.
Inputs may be any that keep to these rules, and one draw needn't show every extreme that they name: `window_ids`: Non-decreasing within each bundle and equal over each 4 consecutive slots; every window lies within one aligned block of 64 slots of a bundle. `image_patches`: multiples of 128; the images of one bundle take at most 512 slots and at least half of them, and in every micro-batch some bundle is full.
All inputs are finite; a program needn't handle non-finite values.
Results may differ from the reference program's by a relative error of at most 0.0053.
Values may be sent and summed in bfloat16 or wider, within the bound.
No kernel may reach another device: no remote copies, remote signals or barrier semaphores. Data moves between devices by JAX's collectives and lax.ppermute only.
A program may use at most 64 MiB of HBM per device.

```python
import math
import jax
import jax.numpy as jnp
from jax import lax

D = 1280
HEADS = 16
WINDOW = 64
IMG_DEV = 4
P_DEV = 512
SAMPLES = 8
GROUP = 32
MICRO = 16
BUNDLES = 512
PATCHES = 262144
IMAGES = 2048


def draw_window_ids(key, part):
    group_slots = P_DEV // 4
    coin_flip = jax.random.randint(jax.random.fold_in(key, 11), (BUNDLES, group_slots), 0, 6)
    slot_index = jnp.arange(group_slots, dtype=jnp.int32)
    forced = (slot_index % (WINDOW // 4) == 0)[None, :]
    finest = (jnp.arange(BUNDLES, dtype=jnp.int32) == 0)[:, None]
    window_starts = jnp.where(forced | finest | (coin_flip == 0), 1, 0).astype(jnp.int32)
    window_index = jnp.cumsum(window_starts, axis=1) - 1
    return jnp.repeat(window_index, 4, axis=1).reshape(BUNDLES * P_DEV).astype(jnp.int32)


def draw_image_patches(key, part):
    unit_count = P_DEV // 128
    lowest = (unit_count + 1) // 2
    totals = jax.random.randint(jax.random.fold_in(key, 21), (BUNDLES,), lowest, unit_count + 1)
    full_member = jax.random.randint(jax.random.fold_in(key, 22), (MICRO,), 0, GROUP)
    bundle_index = jnp.arange(BUNDLES, dtype=jnp.int32)
    totals = jnp.where((bundle_index % GROUP == full_member[bundle_index // GROUP]) | (bundle_index == 0), unit_count, totals)
    slot_choice = jax.random.randint(jax.random.fold_in(key, 23), (BUNDLES, unit_count), 0, IMG_DEV)
    single_slot = jax.random.randint(jax.random.fold_in(key, 24), (), 0, IMG_DEV)
    slot_choice = jnp.where((bundle_index == 0)[:, None], single_slot, slot_choice)
    active = jnp.arange(unit_count, dtype=jnp.int32)[None, :] < totals[:, None]
    matches = (slot_choice[:, :, None] == jnp.arange(IMG_DEV, dtype=jnp.int32)[None, None, :]) & active[:, :, None]
    counts = jnp.sum(matches.astype(jnp.int32), axis=1) * 128
    return counts.reshape(BUNDLES * IMG_DEV).astype(jnp.int32)


def draw_patches(key, part):
    rows = jax.random.normal(jax.random.fold_in(key, 45), (PATCHES, D), jnp.float32)
    return jnp.clip(rows, -6.0, 6.0).astype(jnp.bfloat16)


def draw_w_qkv(key, part):
    unit = 1.0 / math.sqrt(D)
    base = jax.random.normal(jax.random.fold_in(key, 52), (D, 3 * D), jnp.float32)
    return (jnp.clip(base, -3.98, 3.98) * unit).astype(jnp.bfloat16)


def touch_ends(array, key, low, largest):
    extent = array.shape
    index_at = [jax.random.randint(jax.random.fold_in(key, axis), (), 0, extent[axis]) for axis in range(len(extent))]
    array = array.at[tuple(index_at)].set(low)
    longest = extent.index(max(extent))
    index_at[longest] = (index_at[longest] + 1) % extent[longest]
    return array.at[tuple(index_at)].set(largest)


def level_of(stream_key, shape, split, smallest, largest):
    def one(axis_at, parts):
        steps = jax.random.uniform(jax.random.fold_in(jax.random.fold_in(stream_key, 6), axis_at), (parts,), jnp.float32, smallest / len(split), largest / len(split))
        return jnp.repeat(jnp.exp(steps), shape[axis_at] // parts).reshape((-1,) + (1,) * (len(shape) - axis_at - 1))

    level = one(*split[0])
    for cut in split[1:]:
        level = level * one(*cut)
    return level


def bell_draw(rng, extent, scale, limit, split=(), kind=jnp.bfloat16):
    values = scale * jax.random.normal(rng, extent, jnp.float32)
    if split:
        values = values * level_of(rng, extent, split, -0.22, 0.18)
    return jnp.clip(values, -limit, limit).astype(kind)


def setup_inputs(seed: int = 0) -> dict:
    seeds = jax.random.split(jax.random.key(seed), 9)
    return {
        "patches": draw_patches(jax.random.fold_in(seeds[8], 71), 0),
        "attn_gain": jnp.clip(1.0 + 0.15 * jax.random.normal(seeds[1], (D,), jnp.float32), 0.25, 1.75),
        "w_qkv": draw_w_qkv(jax.random.fold_in(seeds[8], 71), 0),
        "w_out": bell_draw(seeds[3], (D, D), D ** -0.5, 0.15625, ((0, 32), (1, 16))),
        "merge_gain": jnp.clip(1.0 + 0.15 * jax.random.normal(seeds[4], (D,), jnp.float32), 0.25, 1.75),
        "window_ids": draw_window_ids(jax.random.fold_in(seeds[8], 71), 0),
        "image_patches": draw_image_patches(jax.random.fold_in(seeds[8], 71), 0),
        "image_sample": touch_ends(jax.random.randint(seeds[7], (IMAGES,), 0, SAMPLES), jax.random.fold_in(seeds[7], 1), 0, SAMPLES - 1).astype(jnp.int32),
    }


epsilon = 1e-06

def normalize(values, gain_row):
    return values * lax.rsqrt(lax.optimization_barrier(jnp.mean(values * values, axis=-1, keepdims=True)) + epsilon) * gain_row

def encode_bundle(patch_rows, window_row, live_row, attn_gain, w_qkv, w_out, merge_gain):
    residual = patch_rows.astype(jnp.float32)
    normed = normalize(residual, attn_gain).astype(jnp.bfloat16)
    qkv = jnp.dot(normed, w_qkv, preferred_element_type=jnp.float32).astype(jnp.bfloat16)
    head_width = D // HEADS
    tile_count = P_DEV // WINDOW

    def split_heads(block):
        return block.reshape(tile_count, WINDOW, HEADS, head_width).astype(jnp.float32)
    queries = split_heads(qkv[:, :D])
    keys_tile = split_heads(qkv[:, D:2 * D])
    values_tile = split_heads(qkv[:, 2 * D:])
    scores = jnp.einsum('tqhd,tkhd->thqk', queries, keys_tile) * (1.0 / math.sqrt(head_width))
    window_tile = window_row.reshape(tile_count, WINDOW)
    live_tile = live_row.reshape(tile_count, WINDOW)
    allowed = (window_tile[:, :, None] == window_tile[:, None, :]) & live_tile[:, None, :]
    scores = jnp.where(allowed[:, None, :, :], scores, -1e+30)
    row_max = lax.optimization_barrier(jnp.max(scores, axis=-1, keepdims=True))
    exponent = jnp.exp(scores - row_max)
    weights = (exponent / lax.optimization_barrier(jnp.sum(exponent, axis=-1, keepdims=True))).astype(jnp.bfloat16)
    context = jnp.einsum('thqk,tkhd->tqhd', weights.astype(jnp.float32), values_tile).reshape(P_DEV, D)
    context = jnp.where(live_row[:, None], context, 0.0).astype(jnp.bfloat16)
    hidden = residual + jnp.dot(context, w_out, preferred_element_type=jnp.float32)
    merged = normalize(hidden, merge_gain).astype(jnp.bfloat16)
    return merged.reshape(P_DEV // 4, 4 * D)

def image_starts(merged_count, samples):
    image_order = jnp.arange(merged_count.shape[0], dtype=jnp.int32)
    ahead = (samples[None, :] < samples[:, None]) | (samples[None, :] == samples[:, None]) & (image_order[None, :] < image_order[:, None])
    return lax.optimization_barrier(jnp.sum(jnp.where(ahead, merged_count[None, :], 0), axis=1)).astype(jnp.int32)

def token_positions(starts, merged_count):
    token_count = P_DEV // 4
    offsets = (jnp.cumsum(merged_count) - merged_count).astype(jnp.int32)
    token_index = jnp.arange(token_count, dtype=jnp.int32)
    inside = (token_index[None, :] >= offsets[:, None]) & (token_index[None, :] < (offsets + merged_count)[:, None])
    position = lax.optimization_barrier(jnp.sum(jnp.where(inside, starts[:, None] + token_index[None, :] - offsets[:, None], 0), axis=0))
    return jnp.where(jnp.any(inside, axis=0), position, -1).astype(jnp.int32)

def reference(patches, attn_gain, w_qkv, w_out, merge_gain, window_ids, image_patches, image_sample):
    token_count = P_DEV // 4
    grouped = (patches.reshape(MICRO, GROUP, P_DEV, D), window_ids.reshape(MICRO, GROUP, P_DEV), image_patches.reshape(MICRO, GROUP, IMG_DEV), image_sample.reshape(MICRO, GROUP, IMG_DEV))

    def one_group(members):
        group_patches, group_windows, group_counts, group_samples = members
        live = jnp.arange(P_DEV, dtype=jnp.int32)[None, :] < lax.optimization_barrier(jnp.sum(group_counts, axis=1))[:, None]

        def encode_member(member):
            return encode_bundle(member[0], member[1], member[2], attn_gain, w_qkv, w_out, merge_gain)
        tokens = lax.map(encode_member, (group_patches, group_windows, live))
        merged_count = (group_counts // 4).astype(jnp.int32)
        starts = image_starts(merged_count.reshape(-1), group_samples.reshape(-1)).reshape(GROUP, IMG_DEV)
        positions = jax.vmap(token_positions)(starts, merged_count)
        positions = jnp.where(positions < 0, GROUP * token_count, positions).astype(jnp.int32)
        sequence = jnp.zeros((GROUP * token_count, 4 * D), jnp.bfloat16)
        sequence = sequence.at[positions.reshape(-1)].set(tokens.reshape(-1, 4 * D), mode='drop')
        return sequence.reshape(token_count, GROUP, 4 * D)
    return lax.map(one_group, grouped)
```

```python
import math

import jax
import jax.numpy as jnp
from jax import lax
from jax.sharding import PartitionSpec as P

HEADS = 16
WINDOW = 64


epsilon = 1e-06


def copy_for_each(x, axis):
    size = lax.axis_size(axis)
    return lax.all_to_all(jnp.broadcast_to(x[None], (size, *x.shape)), axis, 0, 0, tiled=True)


def normalize(values, gain_row):
    return (
        values * lax.rsqrt(jnp.mean(values * values, axis=-1, keepdims=True) + epsilon) * gain_row
    )


def destination_rows(image_patches, image_sample):
    info = copy_for_each(jnp.concatenate([image_patches, image_sample]), "tensor")
    slots = image_patches.shape[0]
    units = info[:, :slots] // 128
    samples = info[:, slots:].reshape(-1)
    flat = units.reshape(-1)
    order = jnp.arange(flat.shape[0], dtype=jnp.int32)
    ahead = (samples[:, None] < samples[None, :]) | (
        (samples[:, None] == samples[None, :]) & (order[:, None] < order[None, :])
    )
    starts = jnp.sum(jnp.where(ahead, flat[:, None], 0), axis=0).reshape(units.shape)
    slot = jnp.arange(slots, dtype=jnp.int32)
    offsets = jnp.sum(jnp.where(slot[:, None] < slot[None, :], units[:, :, None], 0), axis=1)
    unit = slot[None, None, :]
    inside = (unit >= offsets[:, :, None]) & (unit < (offsets + units)[:, :, None])
    row = jnp.sum(jnp.where(inside, (starts - offsets)[:, :, None] + unit, 0), axis=1)
    return jnp.where(jnp.any(inside, axis=1), row, -1)


def body(patches, attn_gain, w_qkv, w_out, merge_gain, window_ids, image_patches, image_sample):
    patch_count, feature_width = patches.shape
    token_count = patch_count // 4
    group_size = lax.axis_size("tensor")
    residual = patches.astype(jnp.float32)
    normed = normalize(residual, attn_gain).astype(jnp.bfloat16)
    qkv_part = w_qkv.shape[1]
    slabs = lax.all_gather(
        jnp.concatenate([w_qkv, w_out], axis=1), ("pipe", "tensor"), axis=0, tiled=True
    ).reshape(lax.axis_size("pipe"), feature_width, -1)
    qkv = (
        jnp.einsum(
            "nk,pkc->npc", normed, slabs[:, :, :qkv_part], preferred_element_type=jnp.float32
        )
        .astype(jnp.bfloat16)
        .reshape(patch_count, 3 * feature_width)
    )
    head_width = feature_width // HEADS
    tile_count = patch_count // WINDOW

    def split_heads(block):
        return block.reshape(tile_count, WINDOW, HEADS, head_width)

    queries = split_heads(qkv[:, :feature_width])
    keys_tile = split_heads(qkv[:, feature_width : 2 * feature_width])
    values_tile = split_heads(qkv[:, 2 * feature_width :])
    scores = jnp.einsum(
        "tqhd,tkhd->thqk", queries, keys_tile, preferred_element_type=jnp.float32
    ) * (1.0 / math.sqrt(head_width))
    live_row = jnp.arange(patch_count, dtype=jnp.int32) < jnp.sum(image_patches)
    window_tile = window_ids.reshape(tile_count, WINDOW)
    live_tile = live_row.reshape(tile_count, WINDOW)
    allowed = (window_tile[:, :, None] == window_tile[:, None, :]) & live_tile[:, None, :]
    scores = jnp.where(allowed[:, None, :, :], scores, -1e30)
    row_max = jnp.max(scores, axis=-1, keepdims=True)
    exponent = jnp.exp(scores - row_max)
    weights = (exponent / jnp.sum(exponent, axis=-1, keepdims=True)).astype(jnp.bfloat16)
    context = jnp.einsum(
        "thqk,tkhd->tqhd", weights, values_tile, preferred_element_type=jnp.float32
    ).reshape(patch_count, feature_width)
    context = jnp.where(live_row[:, None], context, 0.0).astype(jnp.bfloat16)
    attended = jnp.einsum(
        "nk,pkc->npc", context, slabs[:, :, qkv_part:], preferred_element_type=jnp.float32
    ).reshape(patch_count, feature_width)
    hidden = residual + attended
    merged = (
        normalize(hidden, merge_gain).astype(jnp.bfloat16).reshape(token_count, 4 * feature_width)
    )
    outgoing = merged.reshape(token_count // group_size, group_size, 4 * feature_width)
    dest_rows = destination_rows(image_patches, image_sample)
    received = lax.all_to_all(outgoing, "tensor", split_axis=1, concat_axis=0, tiled=True)
    placement = (jnp.arange(token_count, dtype=jnp.int32)[:, None] == dest_rows.reshape(1, token_count)).astype(
        jnp.bfloat16
    )
    placed = jnp.dot(
        placement,
        received.reshape(token_count, 4 * feature_width),
        preferred_element_type=jnp.float32,
    )
    return placed.astype(jnp.bfloat16).reshape(1, token_count, 1, 4 * feature_width)


def solution(mesh):
    return jax.shard_map(
        body,
        mesh=mesh,
        in_specs=(
            P(("pipe", "tensor"), None),
            P(),
            P("tensor", "pipe"),
            P("tensor", "pipe"),
            P(),
            P(("pipe", "tensor")),
            P(("pipe", "tensor")),
            P(("pipe", "tensor")),
        ),
        out_specs=P("pipe", None, "tensor", None),
        check_vma=False,
    )
```

```python
import math

import jax
import jax.numpy as jnp
from jax import lax
from jax.experimental import pallas as pl
from jax.experimental.pallas import tpu as pltpu
from jax.sharding import PartitionSpec as P

HEADS = 16
UNIT = 128

epsilon = 1e-06


def copy_for_each(x, axis):
    size = lax.axis_size(axis)
    return lax.all_to_all(jnp.broadcast_to(x[None], (size, *x.shape)), axis, 0, 0, tiled=True)


def partner_copy(x):
    size = lax.axis_size("pipe")
    return lax.ppermute(x, "pipe", [(p, p ^ 1) for p in range(size)])


def attention_kernel(
    x_ref, gain_ref, w_ref, row_ref, col_ref, out_ref, normed_ref, qkv_ref, *, head_width
):
    step = pl.program_id(0)
    chunk = w_ref.shape[1]
    part = out_ref.shape[1]

    @pl.when(step == 0)
    def _():
        x = x_ref[...].astype(jnp.float32)
        scale = lax.rsqrt(jnp.mean(x * x, axis=-1, keepdims=True) + epsilon)
        normed_ref[...] = (x * scale * gain_ref[...]).astype(jnp.bfloat16)

    qkv_ref[step] = jnp.dot(
        normed_ref[...], w_ref[...], preferred_element_type=jnp.float32
    ).astype(jnp.bfloat16)

    @pl.when(step == pl.num_programs(0) - 1)
    def _():
        def lanes(rows, first, count):
            return jnp.concatenate(
                [
                    qkv_ref[(at * 128) // chunk, rows, pl.ds((at * 128) % chunk, 128)]
                    for at in range(first // 128, (first + count) // 128)
                ],
                axis=1,
            )

        def unit(index, carry):
            rows = pl.ds(pl.multiple_of(index * UNIT, UNIT), UNIT)
            row_id = row_ref[rows, :]
            allowed = row_id == col_ref[pl.ds(index, 1), :]
            columns = [jnp.zeros((UNIT, 128), jnp.float32) for _ in range(part // 128)]
            for head in range(part // head_width):
                first = head * head_width
                base = first // 128 * 128
                count = -(-(first + head_width) // 128) * 128 - base
                lane = lax.broadcasted_iota(jnp.int32, (1, count), 1) + base
                own = (lane >= first) & (lane < first + head_width)
                query = jnp.where(own, lanes(rows, base, count), 0).astype(jnp.bfloat16)
                scores = lax.dot_general(
                    query,
                    lanes(rows, part + base, count),
                    (((1,), (1,)), ((), ())),
                    preferred_element_type=jnp.float32,
                )
                scores = jnp.where(allowed, scores, -1e30)
                highest = jnp.max(scores, axis=-1, keepdims=True)
                weights = jnp.exp((scores - highest) * (1.0 / math.sqrt(head_width)))
                weights = weights * (1.0 / jnp.sum(weights, axis=-1, keepdims=True))
                mixed = jnp.dot(
                    weights.astype(jnp.bfloat16),
                    lanes(rows, 2 * part + base, count),
                    preferred_element_type=jnp.float32,
                )
                for at in range(count // 128):
                    piece = slice(at * 128, at * 128 + 128)
                    place = base // 128 + at
                    columns[place] = jnp.where(own[:, piece], mixed[:, piece], columns[place])
            for place, column in enumerate(columns):
                out_ref[rows, place * 128 : place * 128 + 128] = jnp.where(
                    row_id >= 0, column, 0.0
                ).astype(jnp.bfloat16)
            return carry

        lax.fori_loop(0, out_ref.shape[0] // UNIT, unit, 0)


def half_attention(x, gain, w, row_id, col_id):
    count, width = x.shape
    part = w.shape[1] // 3
    chunk = 384
    head_width = width // HEADS
    whole = lambda *shape: pl.BlockSpec(shape, lambda n: (0,) * len(shape))
    return pl.pallas_call(
        lambda *refs: attention_kernel(*refs, head_width=head_width),
        grid=(w.shape[1] // chunk,),
        in_specs=[
            whole(count, width),
            whole(1, width),
            pl.BlockSpec((width, chunk), lambda n: (0, n)),
            whole(count, 1),
            whole(count // UNIT, UNIT),
        ],
        out_specs=whole(count, part),
        out_shape=jax.ShapeDtypeStruct((count, part), jnp.bfloat16),
        scratch_shapes=[
            pltpu.VMEM((count, width), jnp.bfloat16),
            pltpu.VMEM((w.shape[1] // chunk, count, chunk), jnp.bfloat16),
        ],
        compiler_params=pltpu.CompilerParams(
            dimension_semantics=("arbitrary",), vmem_limit_bytes=28 << 20
        ),
        name="half_attention",
    )(x, gain, w, row_id, col_id)


def merge_kernel(
    core_ref, own_ref, other_ref, w_own_ref, w_other_ref, x_ref, gain_ref, out_ref, hidden_ref, merged_ref
):
    core = core_ref[0]
    count, half = own_ref.shape
    width = 2 * half
    own_rows = pl.ds(pl.multiple_of(core * half, half), half)
    other_rows = pl.ds(pl.multiple_of((1 - core) * half, half), half)
    for w_ref, place in ((w_own_ref, core), (w_other_ref, 1 - core)):
        hidden_ref[place] = jnp.dot(
            own_ref[...], w_ref[own_rows, :], preferred_element_type=jnp.float32
        ) + jnp.dot(other_ref[...], w_ref[other_rows, :], preferred_element_type=jnp.float32)
    low = x_ref[:, :half].astype(jnp.float32) + hidden_ref[0]
    high = x_ref[:, half:].astype(jnp.float32) + hidden_ref[1]
    square = jnp.sum(low * low, axis=-1, keepdims=True) + jnp.sum(
        high * high, axis=-1, keepdims=True
    )
    scale = lax.rsqrt(square * (1.0 / width) + epsilon)
    merged_ref[:, :half] = (low * scale * gain_ref[:, :half]).astype(jnp.bfloat16)
    merged_ref[:, half:] = (high * scale * gain_ref[:, half:]).astype(jnp.bfloat16)
    tokens = out_ref.shape[0]
    units = count // UNIT
    to_row = lax.broadcasted_iota(jnp.int32, (tokens, count), 0)
    from_row = lax.broadcasted_iota(jnp.int32, (tokens, count), 1)
    first_row = (to_row % units) * UNIT + (to_row // units) * 4
    for member in range(4):
        choice = (from_row == first_row + member).astype(jnp.bfloat16)
        out_ref[:, member * width : (member + 1) * width] = jnp.dot(
            choice, merged_ref[...], preferred_element_type=jnp.float32
        ).astype(jnp.bfloat16)


def on_chip(x):
    return pltpu.with_memory_space_constraint(x, pltpu.VMEM)


def in_vmem(count):
    return [pl.BlockSpec(memory_space=pltpu.VMEM)] * count


def merge_tokens(core, own, other, w_own, w_other, x, gain):
    count, width = x.shape
    return pl.pallas_call(
        merge_kernel,
        in_specs=[pl.BlockSpec(memory_space=pltpu.SMEM)] + in_vmem(6),
        out_specs=pl.BlockSpec(memory_space=pltpu.VMEM),
        out_shape=jax.ShapeDtypeStruct((count // 4, 4 * width), jnp.bfloat16),
        scratch_shapes=[
            pltpu.VMEM((2, count, width // 2), jnp.float32),
            pltpu.VMEM((count, width), jnp.bfloat16),
        ],
        compiler_params=pltpu.CompilerParams(vmem_limit_bytes=28 << 20),
        name="merge_tokens",
    )(core, own, on_chip(other), w_own, on_chip(w_other), x, gain)


def unpack_kernel(core_ref, blocks_ref, qkv_ref, out_ref, full_ref, *, qkv_part):
    members, _, columns = blocks_ref.shape
    half = out_ref.shape[1]
    core = core_ref[0]
    for first, last, target in ((0, qkv_part, qkv_ref), (qkv_part, columns, out_ref)):
        pieces = [blocks_ref[p].astype(jnp.float32)[:, first:last] for p in range(members)]
        width = (last - first) * members
        full_ref[:, :width] = jnp.concatenate(pieces, axis=1)
        for at in range(width // (2 * half)):
            start = pl.multiple_of((2 * at + core) * half, 128)
            target[:, at * half : (at + 1) * half] = full_ref[:, pl.ds(start, half)].astype(
                jnp.bfloat16
            )


def unpack_weights(core, blocks, qkv_part):
    members, rows, columns = blocks.shape
    width = members * (columns - qkv_part)
    return pl.pallas_call(
        lambda *refs: unpack_kernel(*refs, qkv_part=qkv_part),
        in_specs=[pl.BlockSpec(memory_space=pltpu.SMEM)] + in_vmem(1),
        out_specs=in_vmem(2),
        out_shape=[
            jax.ShapeDtypeStruct((rows, members * qkv_part // 2), jnp.bfloat16),
            jax.ShapeDtypeStruct((rows, width // 2), jnp.bfloat16),
        ],
        scratch_shapes=[pltpu.VMEM((rows, members * qkv_part), jnp.float32)],
        compiler_params=pltpu.CompilerParams(vmem_limit_bytes=8 << 20),
        name="unpack_weights",
    )(core, on_chip(blocks))


def destination_rows(image_patches, image_sample):
    info = copy_for_each(jnp.concatenate([image_patches, image_sample]), "tensor")
    slots = image_patches.shape[0]
    units = info[:, :slots] // UNIT
    samples = info[:, slots:].reshape(-1)
    flat = units.reshape(-1)
    order = jnp.arange(flat.shape[0], dtype=jnp.int32)
    ahead = (samples[:, None] < samples[None, :]) | (
        (samples[:, None] == samples[None, :]) & (order[:, None] < order[None, :])
    )
    starts = jnp.sum(jnp.where(ahead, flat[:, None], 0), axis=0).reshape(units.shape)
    slot = jnp.arange(slots, dtype=jnp.int32)
    offsets = jnp.sum(jnp.where(slot[:, None] < slot[None, :], units[:, :, None], 0), axis=1)
    unit = slot[None, None, :]
    inside = (unit >= offsets[:, :, None]) & (unit < (offsets + units)[:, :, None])
    row = jnp.sum(jnp.where(inside, (starts - offsets)[:, :, None] + unit, 0), axis=1)
    return jnp.where(jnp.any(inside, axis=1), row, -1)


def body(patches, attn_gain, w_qkv, w_out, merge_gain, window_ids, image_patches, image_sample):
    patch_count, width = patches.shape
    token_count = patch_count // 4
    group_size = lax.axis_size("tensor")
    core = (lax.axis_index("pipe") % 2).astype(jnp.int32).reshape(1)

    blocks = copy_for_each(jnp.concatenate([w_qkv, w_out], axis=1), "pipe")
    qkv_rows, out_rows = unpack_weights(core, blocks, w_qkv.shape[1])
    w_half = lax.all_gather(qkv_rows, "tensor", axis=0, tiled=True)
    out_own = lax.all_gather(out_rows, "tensor", axis=0, tiled=True)

    live = jnp.arange(patch_count, dtype=jnp.int32) < jnp.sum(image_patches)
    ids = jnp.where(live, window_ids, -1)
    other_patches = partner_copy(patches)
    other_ids = partner_copy(ids.reshape(patch_count // UNIT, UNIT)).reshape(patch_count)
    dest_rows = destination_rows(image_patches, image_sample)

    def row_and_column(ids):
        return jnp.where(ids < 0, -2, ids)[:, None], ids.reshape(patch_count // UNIT, UNIT)

    other_patches, other_ids, dest_rows = lax.optimization_barrier(
        (other_patches, other_ids, dest_rows)
    )
    gain = attn_gain[None, :]
    sent = half_attention(other_patches, gain, w_half, *row_and_column(other_ids))
    sent, out_own = lax.optimization_barrier((sent, out_own))
    context_other = partner_copy(sent)
    out_other = partner_copy(out_own)
    context_own = half_attention(patches, gain, w_half, *row_and_column(ids))
    tokens = merge_tokens(
        core,
        context_own,
        context_other,
        out_own,
        out_other,
        patches,
        merge_gain[None, :],
    )
    outgoing = tokens.reshape(group_size, token_count // group_size, 4 * width)
    received = lax.all_to_all(outgoing, "tensor", split_axis=0, concat_axis=0, tiled=True)
    placement = (
        jnp.arange(token_count, dtype=jnp.int32)[:, None] == dest_rows.reshape(1, token_count)
    ).astype(jnp.bfloat16)
    placed = jnp.dot(
        placement, received.reshape(token_count, 4 * width), preferred_element_type=jnp.float32
    )
    return placed.astype(jnp.bfloat16).reshape(1, token_count, 1, 4 * width)


def solution(mesh):
    return jax.shard_map(
        body,
        mesh=mesh,
        in_specs=(
            P(("pipe", "tensor"), None),
            P(),
            P("tensor", "pipe"),
            P("tensor", "pipe"),
            P(),
            P(("pipe", "tensor")),
            P(("pipe", "tensor")),
            P(("pipe", "tensor")),
        ),
        out_specs=P("pipe", None, "tensor", None),
        check_vma=False,
    )
```

```python
import math

import jax
import jax.numpy as jnp
from jax import lax
from jax.experimental import pallas as pl
from jax.experimental.pallas import tpu as pltpu
from jax.sharding import PartitionSpec as P

HEADS = 16
UNIT = 128

epsilon = 1e-06


def copy_for_each(x, axis):
    size = lax.axis_size(axis)
    return lax.all_to_all(jnp.broadcast_to(x[None], (size, *x.shape)), axis, 0, 0, tiled=True)


def partner_copy(x):
    size = lax.axis_size("pipe")
    return lax.ppermute(x, "pipe", [(p, p ^ 1) for p in range(size)])


def attention_kernel(
    x_ref, gain_ref, w_ref, row_ref, col_ref, out_ref, normed_ref, wide_ref, heads_ref, *, head_width
):
    step = pl.program_id(0)
    columns = w_ref.shape[1]
    count, width = x_ref.shape
    head_count = width // head_width
    in_block = columns // head_width

    @pl.when(step == 0)
    def _():
        x = x_ref[...].astype(jnp.float32)
        scale = lax.rsqrt(jnp.mean(x * x, axis=-1, keepdims=True) + epsilon)
        normed_ref[...] = (x * scale * gain_ref[...]).astype(jnp.bfloat16)

    wide_ref[:, :columns] = lax.dot_general(
        normed_ref[...],
        w_ref[0],
        (((1,), (1,)), ((), ())),
        preferred_element_type=jnp.float32,
    ).astype(jnp.bfloat16).astype(jnp.float32)
    lane = lax.broadcasted_iota(jnp.int32, (1, 128), 1)
    for piece in range(in_block):
        part = step * in_block + piece
        offset = jnp.where(part < 2 * head_count, 0, (part - 2 * head_count) * head_width % 128)
        shift = (offset - piece * head_width + 256) % 256
        moved = pltpu.roll(wide_ref[...], shift, axis=1)
        end = offset + head_width
        heads_ref[part] = jnp.where(
            (lane >= offset) & (lane < end),
            moved[:, :128],
            jnp.where(lane < end - 128, moved[:, 128:], 0.0),
        ).astype(jnp.bfloat16)

    @pl.when(step == pl.num_programs(0) - 1)
    def _():
        def unit(index, carry):
            rows = pl.ds(pl.multiple_of(index * UNIT, UNIT), UNIT)
            row_id = row_ref[rows, :]
            live = row_id >= 0
            allowed = row_id == col_ref[pl.ds(index, 1), :]

            def group(number, carry):
                column = jnp.zeros((UNIT, 128), jnp.float32)
                for at in range(8):
                    head = number * 8 + at
                    scores = lax.dot_general(
                        heads_ref[head, rows, :],
                        heads_ref[head_count + head, rows, :],
                        (((1,), (1,)), ((), ())),
                        preferred_element_type=jnp.float32,
                    )
                    scores = jnp.where(allowed, scores, -1e30)
                    highest = jnp.max(scores, axis=-1, keepdims=True)
                    weights = jnp.exp2(
                        (scores - highest) * (1.0 / (math.sqrt(head_width) * math.log(2.0)))
                    )
                    weights = weights * (1.0 / jnp.sum(weights, axis=-1, keepdims=True))
                    mixed = jnp.dot(
                        weights.astype(jnp.bfloat16),
                        heads_ref[2 * head_count + head, rows, :],
                        preferred_element_type=jnp.float32,
                    )
                    first = at * head_width % 128
                    place = at * head_width // 128
                    column = jnp.where(lane >= first, mixed, column)
                    if first + head_width >= 128:
                        start = pl.multiple_of(number * 8 * head_width + place * 128, 128)
                        out_ref[rows, pl.ds(start, 128)] = jnp.where(live, column, 0.0).astype(
                            jnp.bfloat16
                        )
                        column = mixed
                return carry

            return lax.fori_loop(0, head_count // 8, group, carry)

        lax.fori_loop(0, count // UNIT, unit, 0)


def attention(x, gain, slabs, row_id, col_id):
    count, width = x.shape
    blocks, columns, _ = slabs.shape
    head_width = width // HEADS
    whole = lambda *shape: pl.BlockSpec(shape, lambda n: (0,) * len(shape))
    return pl.pallas_call(
        lambda *refs: attention_kernel(*refs, head_width=head_width),
        grid=(blocks,),
        in_specs=[
            whole(count, width),
            whole(1, width),
            pl.BlockSpec((1, columns, width), lambda n: (n, 0, 0)),
            whole(count, 1),
            whole(count // UNIT, UNIT),
        ],
        out_specs=whole(count, width),
        out_shape=jax.ShapeDtypeStruct((count, width), jnp.bfloat16),
        scratch_shapes=[
            pltpu.VMEM((count, width), jnp.bfloat16),
            pltpu.VMEM((count, 256), jnp.float32),
            pltpu.VMEM((3 * HEADS, count, 128), jnp.bfloat16),
        ],
        compiler_params=pltpu.CompilerParams(
            dimension_semantics=("arbitrary",), vmem_limit_bytes=32 << 20
        ),
        name="attention",
    )(x, gain, pltpu.with_memory_space_constraint(slabs, pltpu.HBM), row_id, col_id)


def merge_kernel(
    core_ref, context_ref, w_own_ref, w_other_ref, x_ref, gain_ref, out_ref, hidden_ref, merged_ref
):
    core = core_ref[0]
    count, width = context_ref.shape
    half = width // 2
    for w_ref, place in ((w_own_ref, core), (w_other_ref, 1 - core)):
        hidden_ref[place] = jnp.dot(
            context_ref[...], w_ref[...], preferred_element_type=jnp.float32
        )
    low = x_ref[:, :half].astype(jnp.float32) + hidden_ref[0]
    high = x_ref[:, half:].astype(jnp.float32) + hidden_ref[1]
    square = jnp.sum(low * low, axis=-1, keepdims=True) + jnp.sum(
        high * high, axis=-1, keepdims=True
    )
    scale = lax.rsqrt(square * (1.0 / width) + epsilon)
    merged_ref[:, :half] = (low * scale * gain_ref[:, :half]).astype(jnp.bfloat16)
    merged_ref[:, half:] = (high * scale * gain_ref[:, half:]).astype(jnp.bfloat16)
    tokens = out_ref.shape[0]
    units = count // UNIT
    to_row = lax.broadcasted_iota(jnp.int32, (tokens, count), 0)
    from_row = lax.broadcasted_iota(jnp.int32, (tokens, count), 1)
    first_row = (to_row % units) * UNIT + (to_row // units) * 4
    for member in range(4):
        choice = (from_row == first_row + member).astype(jnp.bfloat16)
        out_ref[:, member * width : (member + 1) * width] = jnp.dot(
            choice, merged_ref[...], preferred_element_type=jnp.float32
        ).astype(jnp.bfloat16)


def on_chip(x):
    return pltpu.with_memory_space_constraint(x, pltpu.VMEM)


def in_vmem(count):
    return [pl.BlockSpec(memory_space=pltpu.VMEM)] * count


def merge_tokens(core, context, w_own, w_other, x, gain):
    count, width = x.shape
    return pl.pallas_call(
        merge_kernel,
        in_specs=[pl.BlockSpec(memory_space=pltpu.SMEM)] + in_vmem(5),
        out_specs=pl.BlockSpec(memory_space=pltpu.VMEM),
        out_shape=jax.ShapeDtypeStruct((count // 4, 4 * width), jnp.bfloat16),
        scratch_shapes=[
            pltpu.VMEM((2, count, width // 2), jnp.float32),
            pltpu.VMEM((count, width), jnp.bfloat16),
        ],
        compiler_params=pltpu.CompilerParams(vmem_limit_bytes=28 << 20),
        name="merge_tokens",
    )(core, context, on_chip(w_own), on_chip(w_other), x, gain)


def destination_rows(units, samples):
    slots = units.shape[1]
    samples = samples.reshape(-1)
    flat = units.reshape(-1)
    order = jnp.arange(flat.shape[0], dtype=jnp.int32)
    ahead = (samples[:, None] < samples[None, :]) | (
        (samples[:, None] == samples[None, :]) & (order[:, None] < order[None, :])
    )
    starts = jnp.sum(jnp.where(ahead, flat[:, None], 0), axis=0).reshape(units.shape)
    slot = jnp.arange(slots, dtype=jnp.int32)
    offsets = jnp.sum(jnp.where(slot[:, None] < slot[None, :], units[:, :, None], 0), axis=1)
    unit = slot[None, None, :]
    inside = (unit >= offsets[:, :, None]) & (unit < (offsets + units)[:, :, None])
    row = jnp.sum(jnp.where(inside, (starts - offsets)[:, :, None] + unit, 0), axis=1)
    return jnp.where(jnp.any(inside, axis=1), row, -1)


def body(patches, attn_gain, w_qkv, w_out, merge_gain, window_ids, image_patches, image_sample):
    patch_count, width = patches.shape
    token_count = patch_count // 4
    group_size = lax.axis_size("tensor")
    core = (lax.axis_index("pipe") % 2).astype(jnp.int32).reshape(1)

    half = width // 2
    slots = image_patches.shape[0]
    row_count, qkv_part = w_qkv.shape

    info = jnp.concatenate([image_patches // UNIT, image_sample]).astype(jnp.bfloat16)
    info = jnp.broadcast_to(info[None], (row_count, 2 * slots))
    rows = copy_for_each(jnp.concatenate([w_qkv, info], axis=1), "tensor")
    slab = rows[:, :, :qkv_part].reshape(width, qkv_part).T
    slabs = lax.all_gather(slab, "pipe", axis=0, tiled=False)
    info = rows[:, 0, qkv_part:].astype(jnp.int32)
    dest_rows = destination_rows(info[:, :slots], info[:, slots:])

    slab, w_out = lax.optimization_barrier((slab, w_out))
    blocks = copy_for_each(w_out, "pipe")
    out_rows = jnp.moveaxis(blocks, 0, 1).reshape(row_count, 2, half)
    out_rows = lax.dynamic_index_in_dim(out_rows, core[0], axis=1, keepdims=False)
    out_own = copy_for_each(out_rows, "tensor").reshape(width, half)
    out_other = partner_copy(out_own)

    live = jnp.arange(patch_count, dtype=jnp.int32) < jnp.sum(image_patches)
    ids = jnp.where(live, window_ids, -1)
    ids, dest_rows, out_own = lax.optimization_barrier((ids, dest_rows, out_own))
    context = attention(
        patches,
        attn_gain[None, :],
        slabs,
        jnp.where(ids < 0, -2, ids)[:, None],
        ids.reshape(patch_count // UNIT, UNIT),
    )
    tokens = merge_tokens(core, context, out_own, out_other, patches, merge_gain[None, :])
    outgoing = tokens.reshape(group_size, token_count // group_size, 4 * width)
    received = lax.all_to_all(outgoing, "tensor", split_axis=0, concat_axis=0, tiled=True)
    placement = (
        jnp.arange(token_count, dtype=jnp.int32)[:, None] == dest_rows.reshape(1, token_count)
    ).astype(jnp.bfloat16)
    placed = jnp.dot(
        placement, received.reshape(token_count, 4 * width), preferred_element_type=jnp.float32
    )
    return placed.astype(jnp.bfloat16).reshape(1, token_count, 1, 4 * width)


def solution(mesh):
    return jax.shard_map(
        body,
        mesh=mesh,
        in_specs=(
            P(("pipe", "tensor"), None),
            P(),
            P("tensor", "pipe"),
            P("tensor", "pipe"),
            P(),
            P(("pipe", "tensor")),
            P(("pipe", "tensor")),
            P(("pipe", "tensor")),
        ),
        out_specs=P("pipe", None, "tensor", None),
        check_vma=False,
    )
```

```python
import math

import jax
import jax.numpy as jnp
from jax import lax
from jax.experimental import pallas as pl
from jax.experimental.pallas import tpu as pltpu
from jax.sharding import PartitionSpec as P

HEADS = 16
UNIT = 128

epsilon = 1e-06


def copy_for_each(x, axis):
    size = lax.axis_size(axis)
    return lax.all_to_all(jnp.broadcast_to(x[None], (size, *x.shape)), axis, 0, 0, tiled=True)


def partner_copy(x):
    size = lax.axis_size("pipe")
    return lax.ppermute(x, "pipe", [(p, p ^ 1) for p in range(size)])


def attention_kernel(
    x_ref, gain_ref, w_ref, key_ref, query_ref, out_ref, normed_ref, qkv_ref, context_ref, *, head_width
):
    step = pl.program_id(0)
    chunk = w_ref.shape[0]
    count, width = x_ref.shape
    head_count = width // head_width
    chunks = 3 * width // chunk

    @pl.when(step == 0)
    def _():
        x = x_ref[...].astype(jnp.float32)
        scale = lax.rsqrt(jnp.mean(x * x, axis=-1, keepdims=True) + epsilon)
        normed_ref[...] = (x * scale * gain_ref[...]).astype(jnp.bfloat16).T

    @pl.when(step < chunks)
    def _():
        qkv_ref[pl.ds(pl.multiple_of(step * chunk, chunk), chunk), :] = jnp.dot(
            w_ref[...], normed_ref[...], preferred_element_type=jnp.float32
        ).astype(jnp.bfloat16)

    @pl.when(step >= chunks)
    def _():
        unit = step - chunks
        patches = pl.ds(pl.multiple_of(unit * UNIT, UNIT), UNIT)
        query_id = query_ref[pl.ds(unit, 1), :]
        allowed = key_ref[patches, :] == query_id
        for head in range(head_count):
            query, key, value = (
                qkv_ref[part * width + head * head_width : part * width + (head + 1) * head_width, patches]
                for part in range(3)
            )
            scores = lax.dot_general(
                key, query, (((0,), (0,)), ((), ())), preferred_element_type=jnp.float32
            )
            scores = jnp.where(allowed, scores, -1e30)
            highest = jnp.max(scores, axis=0, keepdims=True)
            weights = jnp.exp2(
                (scores - highest) * (1.0 / (math.sqrt(head_width) * math.log(2.0)))
            )
            total = jnp.sum(weights, axis=0, keepdims=True)
            weights = weights * jnp.where(query_id >= 0, 1.0 / total, 0.0)
            context_ref[head * head_width : (head + 1) * head_width, :] = jnp.dot(
                value, weights.astype(jnp.bfloat16), preferred_element_type=jnp.float32
            ).astype(jnp.bfloat16)
        out_ref[...] = context_ref[...].T


def attention(x, gain, w, key_id, query_id):
    count, width = x.shape
    chunk = 3 * width // 4
    units = count // UNIT
    whole = lambda *shape: pl.BlockSpec(shape, lambda n: (0,) * len(shape))
    return pl.pallas_call(
        lambda *refs: attention_kernel(*refs, head_width=width // HEADS),
        grid=(4 + units,),
        in_specs=[
            whole(count, width),
            whole(1, width),
            pl.BlockSpec((chunk, width), lambda n: (jnp.minimum(n, 3), 0)),
            whole(count, 1),
            whole(units, UNIT),
        ],
        out_specs=pl.BlockSpec((UNIT, width), lambda n: (jnp.maximum(n - 4, 0), 0)),
        out_shape=jax.ShapeDtypeStruct((count, width), jnp.bfloat16),
        scratch_shapes=[
            pltpu.VMEM((width, count), jnp.bfloat16),
            pltpu.VMEM((3 * width, count), jnp.bfloat16),
            pltpu.VMEM((width, UNIT), jnp.bfloat16),
        ],
        compiler_params=pltpu.CompilerParams(
            dimension_semantics=("arbitrary",), vmem_limit_bytes=32 << 20
        ),
        name="attention",
    )(x, gain, pltpu.with_memory_space_constraint(w, pltpu.HBM), key_id, query_id)


def merge_kernel(
    core_ref, context_ref, w_own_ref, w_other_ref, x_ref, gain_ref, out_ref, hidden_ref, merged_ref
):
    core = core_ref[0]
    count, width = context_ref.shape
    half = width // 2
    for w_ref, place in ((w_own_ref, core), (w_other_ref, 1 - core)):
        hidden_ref[place] = jnp.dot(
            context_ref[...], w_ref[...], preferred_element_type=jnp.float32
        )
    low = x_ref[:, :half].astype(jnp.float32) + hidden_ref[0]
    high = x_ref[:, half:].astype(jnp.float32) + hidden_ref[1]
    square = jnp.sum(low * low, axis=-1, keepdims=True) + jnp.sum(
        high * high, axis=-1, keepdims=True
    )
    scale = lax.rsqrt(square * (1.0 / width) + epsilon)
    merged_ref[:, :half] = (low * scale * gain_ref[:, :half]).astype(jnp.bfloat16)
    merged_ref[:, half:] = (high * scale * gain_ref[:, half:]).astype(jnp.bfloat16)
    tokens = out_ref.shape[0]
    units = count // UNIT
    to_row = lax.broadcasted_iota(jnp.int32, (tokens, count), 0)
    from_row = lax.broadcasted_iota(jnp.int32, (tokens, count), 1)
    first_row = (to_row % units) * UNIT + (to_row // units) * 4
    for member in range(4):
        choice = (from_row == first_row + member).astype(jnp.bfloat16)
        out_ref[:, member * width : (member + 1) * width] = jnp.dot(
            choice, merged_ref[...], preferred_element_type=jnp.float32
        ).astype(jnp.bfloat16)


def on_chip(x):
    return pltpu.with_memory_space_constraint(x, pltpu.VMEM)


def in_vmem(count):
    return [pl.BlockSpec(memory_space=pltpu.VMEM)] * count


def merge_tokens(core, context, w_own, w_other, x, gain):
    count, width = x.shape
    return pl.pallas_call(
        merge_kernel,
        in_specs=[pl.BlockSpec(memory_space=pltpu.SMEM)] + in_vmem(5),
        out_specs=pl.BlockSpec(memory_space=pltpu.VMEM),
        out_shape=jax.ShapeDtypeStruct((count // 4, 4 * width), jnp.bfloat16),
        scratch_shapes=[
            pltpu.VMEM((2, count, width // 2), jnp.float32),
            pltpu.VMEM((count, width), jnp.bfloat16),
        ],
        compiler_params=pltpu.CompilerParams(vmem_limit_bytes=28 << 20),
        name="merge_tokens",
    )(core, context, on_chip(w_own), on_chip(w_other), x, gain)


def destination_rows(units, samples):
    slots = units.shape[1]
    samples = samples.reshape(-1)
    flat = units.reshape(-1)
    order = jnp.arange(flat.shape[0], dtype=jnp.int32)
    ahead = (samples[:, None] < samples[None, :]) | (
        (samples[:, None] == samples[None, :]) & (order[:, None] < order[None, :])
    )
    starts = jnp.sum(jnp.where(ahead, flat[:, None], 0), axis=0).reshape(units.shape)
    slot = jnp.arange(slots, dtype=jnp.int32)
    offsets = jnp.sum(jnp.where(slot[:, None] < slot[None, :], units[:, :, None], 0), axis=1)
    unit = slot[None, None, :]
    inside = (unit >= offsets[:, :, None]) & (unit < (offsets + units)[:, :, None])
    row = jnp.sum(jnp.where(inside, (starts - offsets)[:, :, None] + unit, 0), axis=1)
    return jnp.where(jnp.any(inside, axis=1), row, -1)


def body(patches, attn_gain, w_qkv, w_out, merge_gain, window_ids, image_patches, image_sample):
    patch_count, width = patches.shape
    token_count = patch_count // 4
    group_size = lax.axis_size("tensor")
    core = (lax.axis_index("pipe") % 2).astype(jnp.int32).reshape(1)

    half = width // 2
    slots = image_patches.shape[0]
    row_count, qkv_part = w_qkv.shape

    info = jnp.concatenate([image_patches // UNIT, image_sample]).astype(jnp.bfloat16)
    info = jnp.broadcast_to(info[None], (row_count, 2 * slots))
    rows = copy_for_each(jnp.concatenate([w_qkv, info], axis=1), "tensor")
    slab = rows[:, :, :qkv_part].reshape(width, qkv_part).T
    w_all = lax.all_gather(slab, "pipe", axis=0, tiled=True)
    info = rows[:, 0, qkv_part:].astype(jnp.int32)
    dest_rows = destination_rows(info[:, :slots], info[:, slots:])

    blocks = copy_for_each(w_out, "pipe")
    out_rows = jnp.moveaxis(blocks, 0, 1).reshape(row_count, 2, half)
    out_rows = lax.dynamic_index_in_dim(out_rows, core[0], axis=1, keepdims=False)
    out_own = copy_for_each(out_rows, "tensor").reshape(width, half)
    out_other = partner_copy(out_own)

    live = jnp.arange(patch_count, dtype=jnp.int32) < jnp.sum(image_patches)
    ids = jnp.where(live, window_ids, -1)
    ids, dest_rows = lax.optimization_barrier((ids, dest_rows))
    context = attention(
        patches,
        attn_gain[None, :],
        w_all,
        ids[:, None],
        jnp.where(ids < 0, -2, ids).reshape(patch_count // UNIT, UNIT),
    )
    tokens = merge_tokens(core, context, out_own, out_other, patches, merge_gain[None, :])
    outgoing = tokens.reshape(group_size, token_count // group_size, 4 * width)
    received = lax.all_to_all(outgoing, "tensor", split_axis=0, concat_axis=0, tiled=True)
    placement = (
        jnp.arange(token_count, dtype=jnp.int32)[:, None] == dest_rows.reshape(1, token_count)
    ).astype(jnp.bfloat16)
    placed = jnp.dot(
        placement, received.reshape(token_count, 4 * width), preferred_element_type=jnp.float32
    )
    return placed.astype(jnp.bfloat16).reshape(1, token_count, 1, 4 * width)


def solution(mesh):
    return jax.shard_map(
        body,
        mesh=mesh,
        in_specs=(
            P(("pipe", "tensor"), None),
            P(),
            P("tensor", "pipe"),
            P("tensor", "pipe"),
            P(),
            P(("pipe", "tensor")),
            P(("pipe", "tensor")),
            P(("pipe", "tensor")),
        ),
        out_specs=P("pipe", None, "tensor", None),
        check_vma=False,
    )
```

```python
import math

import jax
import jax.numpy as jnp
from jax import lax
from jax.experimental import pallas as pl
from jax.experimental.pallas import tpu as pltpu
from jax.sharding import PartitionSpec as P

HEADS = 16
UNIT = 128

epsilon = 1e-06


def copy_for_each(x, axis):
    size = lax.axis_size(axis)
    return lax.all_to_all(jnp.broadcast_to(x[None], (size, *x.shape)), axis, 0, 0, tiled=True)


def partner_copy(x):
    size = lax.axis_size("pipe")
    return lax.ppermute(x, "pipe", [(p, p ^ 1) for p in range(size)])


def chip_copy(x, chips):
    size = lax.axis_size("pipe")
    return lax.ppermute(x, "pipe", [(p, (p + 2 * chips) % size) for p in range(size)])


def ring_project(slab, normed, w_out, core, early):
    rows = slab.shape[0]
    size = lax.axis_size("pipe")
    place = lax.axis_index("pipe").astype(jnp.int32)
    together = lax.optimization_barrier

    def firsts(pieces):
        owners = [(place + owner, offset) for owner, offset in pieces]
        owners += [((place ^ 1) + owner, offset) for owner, offset in pieces]
        return jnp.stack([((owner + size) % size) * rows + offset for owner, offset in owners])

    cut = rows * 2 // 3
    near = [(0, 0)], [(-2, 0), (2, 0)], [(-4, 0), (4, 0)], [(-6, 0), (6, 0)], [(8, 0), (8, cut)]
    a1, b1 = chip_copy(slab, 1), chip_copy(slab, -1)
    blocks = copy_for_each(w_out, "pipe")
    other = partner_copy(slab)
    a1, b1, other, normed, blocks = together((a1, b1, other, normed, blocks))

    a2, b2 = chip_copy(a1, 1), chip_copy(b1, -1)
    pa1, pb1 = partner_copy(a1), partner_copy(b1)
    half = blocks.shape[0] * blocks.shape[2] // 2
    out_rows = jnp.moveaxis(blocks, 0, 1).reshape(blocks.shape[1], 2, half)
    out_rows = lax.dynamic_index_in_dim(out_rows, core[0], axis=1, keepdims=False)
    out_own = copy_for_each(out_rows, "tensor")
    buffer = project(normed, [slab, other], firsts(near[0]), None)
    a2, b2, pa1, pb1, buffer, early = together((a2, b2, pa1, pb1, buffer, early))

    a3, b3 = chip_copy(a2, 1), chip_copy(b2, -1)
    pa2, pb2 = partner_copy(a2), partner_copy(b2)
    buffer = project(normed, [a1, b1, pa1, pb1], firsts(near[1]), buffer)
    a3, b3, pa2, pb2, buffer = together((a3, b3, pa2, pb2, buffer))

    a4, b4 = chip_copy(a3[:cut], 1), chip_copy(b3[cut:], -1)
    pa3, pb3 = partner_copy(a3), partner_copy(b3)
    buffer = project(normed, [a2, b2, pa2, pb2], firsts(near[2]), buffer)
    a4, b4, pa3, pb3, buffer = together((a4, b4, pa3, pb3, buffer))

    pa4, pb4 = partner_copy(a4), partner_copy(b4)
    buffer = project(normed, [a3, b3, pa3, pb3], firsts(near[3]), buffer)
    pa4, pb4, buffer, out_own = together((pa4, pb4, buffer, out_own))
    buffer = project(normed, [a4, b4, pa4, pb4], firsts(near[4]), buffer)
    return buffer, out_own.reshape(-1, half), early


def on_chip(x):
    return pltpu.with_memory_space_constraint(x, pltpu.VMEM)


def in_hbm(x):
    return pltpu.with_memory_space_constraint(x, pltpu.HBM)


def in_vmem(count):
    return [pl.BlockSpec(memory_space=pltpu.VMEM)] * count


def normalize_kernel(x_ref, gain_ref, out_ref):
    x = x_ref[...].astype(jnp.float32)
    scale = lax.rsqrt(jnp.mean(x * x, axis=-1, keepdims=True) + epsilon)
    out_ref[...] = (x * scale * gain_ref[...]).astype(jnp.bfloat16).T


def normalize_rows(x, gain):
    return pl.pallas_call(
        normalize_kernel,
        in_specs=in_vmem(2),
        out_specs=pl.BlockSpec(memory_space=pltpu.VMEM),
        out_shape=jax.ShapeDtypeStruct((x.shape[1], x.shape[0]), jnp.bfloat16),
        compiler_params=pltpu.CompilerParams(vmem_limit_bytes=16 << 20),
        name="normalize_rows",
    )(x, gain)


def project_kernel(first_ref, normed_ref, *refs, pieces, aliased):
    slab_refs = refs[:pieces]
    out_ref, part_ref, sems = refs[pieces + aliased :]
    copies = []
    at = 0
    for piece, slab_ref in enumerate(slab_refs):
        rows = slab_ref.shape[0]
        part_ref[at : at + rows, :] = jnp.dot(
            slab_ref[...], normed_ref[...], preferred_element_type=jnp.float32
        ).astype(jnp.bfloat16)
        first = pl.multiple_of(first_ref[piece], 80)
        copies.append(
            pltpu.make_async_copy(
                part_ref.at[at : at + rows, :], out_ref.at[pl.ds(first, rows), :], sems.at[piece]
            )
        )
        copies[-1].start()
        at += rows
    for copy in copies:
        copy.wait()


def project(normed, slabs, firsts, buffer):
    width, count = normed.shape
    aliased = buffer is not None
    rows = sum(slab.shape[0] for slab in slabs)
    return pl.pallas_call(
        lambda *refs: project_kernel(*refs, pieces=len(slabs), aliased=aliased),
        in_specs=[pl.BlockSpec(memory_space=pltpu.SMEM)]
        + in_vmem(1 + len(slabs))
        + [pl.BlockSpec(memory_space=pltpu.HBM)] * aliased,
        out_specs=pl.BlockSpec(memory_space=pltpu.HBM),
        out_shape=pltpu.HBM((3 * width, count), jnp.bfloat16),
        scratch_shapes=[
            pltpu.VMEM((rows, count), jnp.bfloat16),
            pltpu.SemaphoreType.DMA((len(slabs),)),
        ],
        input_output_aliases={2 + len(slabs): 0} if aliased else {},
        compiler_params=pltpu.CompilerParams(vmem_limit_bytes=16 << 20),
        name="project",
    )(firsts, normed, *slabs, *([in_hbm(buffer)] if aliased else []))


def attention_kernel(qkv_ref, key_ref, query_ref, out_ref, context_ref, *, head_width):
    width = out_ref.shape[1]
    query_id = query_ref[pl.ds(pl.program_id(0), 1), :]
    allowed = key_ref[...] == query_id
    for head in range(width // head_width):
        query, key, value = (
            qkv_ref[part * width + head * head_width : part * width + (head + 1) * head_width, :]
            for part in range(3)
        )
        scores = lax.dot_general(
            key, query, (((0,), (0,)), ((), ())), preferred_element_type=jnp.float32
        )
        scores = jnp.where(allowed, scores, -1e30)
        highest = jnp.max(scores, axis=0, keepdims=True)
        weights = jnp.exp2((scores - highest) * (1.0 / (math.sqrt(head_width) * math.log(2.0))))
        total = jnp.sum(weights, axis=0, keepdims=True)
        weights = weights * jnp.where(query_id >= 0, 1.0 / total, 0.0)
        context_ref[head * head_width : (head + 1) * head_width, :] = jnp.dot(
            value, weights.astype(jnp.bfloat16), preferred_element_type=jnp.float32
        ).astype(jnp.bfloat16)
    out_ref[...] = context_ref[...].T


def attention(qkv, key_id, query_id):
    width, count = qkv.shape[0] // 3, qkv.shape[1]
    units = count // UNIT
    return pl.pallas_call(
        lambda *refs: attention_kernel(*refs, head_width=width // HEADS),
        grid=(units,),
        in_specs=[
            pl.BlockSpec((3 * width, UNIT), lambda n: (0, n)),
            pl.BlockSpec((UNIT, 1), lambda n: (n, 0)),
            pl.BlockSpec((units, UNIT), lambda n: (0, 0)),
        ],
        out_specs=pl.BlockSpec((UNIT, width), lambda n: (n, 0)),
        out_shape=jax.ShapeDtypeStruct((count, width), jnp.bfloat16),
        scratch_shapes=[pltpu.VMEM((width, UNIT), jnp.bfloat16)],
        compiler_params=pltpu.CompilerParams(
            dimension_semantics=("arbitrary",), vmem_limit_bytes=16 << 20
        ),
        name="attention",
    )(in_hbm(qkv), key_id, query_id)


def merge_kernel(
    core_ref, context_ref, w_own_ref, w_other_ref, x_ref, gain_ref, out_ref, hidden_ref, merged_ref
):
    core = core_ref[0]
    count, width = context_ref.shape
    half = width // 2
    for w_ref, place in ((w_own_ref, core), (w_other_ref, 1 - core)):
        hidden_ref[place] = jnp.dot(
            context_ref[...], w_ref[...], preferred_element_type=jnp.float32
        )
    low = x_ref[:, :half].astype(jnp.float32) + hidden_ref[0]
    high = x_ref[:, half:].astype(jnp.float32) + hidden_ref[1]
    square = jnp.sum(low * low, axis=-1, keepdims=True) + jnp.sum(
        high * high, axis=-1, keepdims=True
    )
    scale = lax.rsqrt(square * (1.0 / width) + epsilon)
    merged_ref[:, :half] = (low * scale * gain_ref[:, :half]).astype(jnp.bfloat16)
    merged_ref[:, half:] = (high * scale * gain_ref[:, half:]).astype(jnp.bfloat16)
    tokens = out_ref.shape[0]
    units = count // UNIT
    to_row = lax.broadcasted_iota(jnp.int32, (tokens, count), 0)
    from_row = lax.broadcasted_iota(jnp.int32, (tokens, count), 1)
    first_row = (to_row % units) * UNIT + (to_row // units) * 4
    for member in range(4):
        choice = (from_row == first_row + member).astype(jnp.bfloat16)
        out_ref[:, member * width : (member + 1) * width] = jnp.dot(
            choice, merged_ref[...], preferred_element_type=jnp.float32
        ).astype(jnp.bfloat16)


def merge_tokens(core, context, w_own, w_other, x, gain):
    count, width = x.shape
    return pl.pallas_call(
        merge_kernel,
        in_specs=[pl.BlockSpec(memory_space=pltpu.SMEM)] + in_vmem(5),
        out_specs=pl.BlockSpec(memory_space=pltpu.VMEM),
        out_shape=jax.ShapeDtypeStruct((count // 4, 4 * width), jnp.bfloat16),
        scratch_shapes=[
            pltpu.VMEM((2, count, width // 2), jnp.float32),
            pltpu.VMEM((count, width), jnp.bfloat16),
        ],
        compiler_params=pltpu.CompilerParams(vmem_limit_bytes=28 << 20),
        name="merge_tokens",
    )(core, context, on_chip(w_own), on_chip(w_other), x, gain)


def destination_rows(units, samples):
    slots = units.shape[1]
    samples = samples.reshape(-1)
    flat = units.reshape(-1)
    order = jnp.arange(flat.shape[0], dtype=jnp.int32)
    ahead = (samples[:, None] < samples[None, :]) | (
        (samples[:, None] == samples[None, :]) & (order[:, None] < order[None, :])
    )
    starts = jnp.sum(jnp.where(ahead, flat[:, None], 0), axis=0).reshape(units.shape)
    slot = jnp.arange(slots, dtype=jnp.int32)
    offsets = jnp.sum(jnp.where(slot[:, None] < slot[None, :], units[:, :, None], 0), axis=1)
    unit = slot[None, None, :]
    inside = (unit >= offsets[:, :, None]) & (unit < (offsets + units)[:, :, None])
    row = jnp.sum(jnp.where(inside, (starts - offsets)[:, :, None] + unit, 0), axis=1)
    return jnp.where(jnp.any(inside, axis=1), row, -1)


def body(patches, attn_gain, w_qkv, w_out, merge_gain, window_ids, image_patches, image_sample):
    patch_count, width = patches.shape
    token_count = patch_count // 4
    group_size = lax.axis_size("tensor")
    core = (lax.axis_index("pipe") % 2).astype(jnp.int32).reshape(1)

    slots = image_patches.shape[0]
    row_count, qkv_part = w_qkv.shape

    info = jnp.concatenate([image_patches // UNIT, image_sample]).astype(jnp.bfloat16)
    info = jnp.broadcast_to(info[None], (row_count, 2 * slots))
    rows = copy_for_each(jnp.concatenate([w_qkv, info], axis=1), "tensor")
    slab = rows[:, :, :qkv_part].reshape(width, qkv_part).T
    info = rows[:, 0, qkv_part:].astype(jnp.int32)
    dest_rows = destination_rows(info[:, :slots], info[:, slots:])

    slab, w_out = lax.optimization_barrier((slab, w_out))
    normed = normalize_rows(patches, attn_gain[None, :])
    live = jnp.arange(patch_count, dtype=jnp.int32) < jnp.sum(image_patches)
    key_id = jnp.where(live, window_ids, -1)[:, None]
    query_id = jnp.where(live, window_ids, -2).reshape(patch_count // UNIT, UNIT)
    qkv, out_own, (key_id, query_id, dest_rows) = ring_project(
        slab, normed, w_out, core, (key_id, query_id, dest_rows)
    )
    out_other = partner_copy(out_own)
    context = attention(qkv, key_id, query_id)
    tokens = merge_tokens(core, context, out_own, out_other, patches, merge_gain[None, :])
    outgoing = tokens.reshape(group_size, token_count // group_size, 4 * width)
    received = lax.all_to_all(outgoing, "tensor", split_axis=0, concat_axis=0, tiled=True)
    placement = (
        jnp.arange(token_count, dtype=jnp.int32)[:, None] == dest_rows.reshape(1, token_count)
    ).astype(jnp.bfloat16)
    placed = jnp.dot(
        placement, received.reshape(token_count, 4 * width), preferred_element_type=jnp.float32
    )
    return placed.astype(jnp.bfloat16).reshape(1, token_count, 1, 4 * width)


def solution(mesh):
    return jax.shard_map(
        body,
        mesh=mesh,
        in_specs=(
            P(("pipe", "tensor"), None),
            P(),
            P("tensor", "pipe"),
            P("tensor", "pipe"),
            P(),
            P(("pipe", "tensor")),
            P(("pipe", "tensor")),
            P(("pipe", "tensor")),
        ),
        out_specs=P("pipe", None, "tensor", None),
        check_vma=False,
    )
```

```python
import math

import jax
import jax.numpy as jnp
from jax import lax
from jax.experimental import pallas as pl
from jax.experimental.pallas import tpu as pltpu
from jax.sharding import PartitionSpec as P

HEADS = 16
UNIT = 128

epsilon = 1e-06


def copy_for_each(x, axis):
    size = lax.axis_size(axis)
    return lax.all_to_all(jnp.broadcast_to(x[None], (size, *x.shape)), axis, 0, 0, tiled=True)


def partner_copy(x):
    size = lax.axis_size("pipe")
    return lax.ppermute(x, "pipe", [(p, p ^ 1) for p in range(size)])


def chip_copy(x, chips):
    size = lax.axis_size("pipe")
    return lax.ppermute(x, "pipe", [(p, (p + 2 * chips) % size) for p in range(size)])


def ring_project(slab, patches, gain, w_out, core, early):
    rows = slab.shape[0]
    size = lax.axis_size("pipe")
    place = lax.axis_index("pipe").astype(jnp.int32)
    together = lax.optimization_barrier
    other = partner_copy(patches)
    normed = normalize_rows(patches, other, gain)

    a1, b1 = chip_copy(slab, 1), chip_copy(slab, -1)
    blocks = copy_for_each(w_out, "pipe")
    a1, b1, normed, blocks, early = together((a1, b1, normed, blocks, early))

    a2, b2 = chip_copy(a1, 1), chip_copy(b1, -1)
    half = blocks.shape[0] * blocks.shape[2] // 2
    out_rows = jnp.moveaxis(blocks, 0, 1).reshape(blocks.shape[1], 2, half)
    out_rows = lax.dynamic_index_in_dim(out_rows, core[0], axis=1, keepdims=False)
    out_own = copy_for_each(out_rows, "tensor")
    a2, b2 = together((a2, b2))

    a3, b3 = chip_copy(a2, 1), chip_copy(b2, -1)
    own1, sent1 = project(normed, [slab, a1, b1, a2, b2])
    a3, b3, own1, sent1 = together((a3, b3, own1, sent1))

    a4 = chip_copy(a3, 1)
    got1 = partner_copy(sent1)
    own2, sent2 = project(normed, [a3, b3])
    a4, own2, sent2 = together((a4, own2, sent2))

    own3, sent3 = project(normed, [a4])
    got2, got3 = partner_copy(sent2), partner_copy(sent3)
    got3, out_own = together((got3, out_own))
    owners = [0, -2, 2, -4, 4, -6, 6, 8]
    owners = [place + owner for owner in owners] + [(place ^ 1) + owner for owner in owners]
    firsts = jnp.stack([(owner + size) % size * rows for owner in owners])
    return (firsts, own1, own2, own3, got1, got2, got3), out_own.reshape(-1, half), early


def on_chip(x):
    return pltpu.with_memory_space_constraint(x, pltpu.VMEM)


def in_hbm(x):
    return pltpu.with_memory_space_constraint(x, pltpu.HBM)


def in_vmem(count):
    return [pl.BlockSpec(memory_space=pltpu.VMEM)] * count


def normalize_kernel(x_ref, other_ref, gain_ref, out_ref):
    count = x_ref.shape[0]
    for at, ref in enumerate((x_ref, other_ref)):
        x = ref[...].astype(jnp.float32)
        scale = lax.rsqrt(jnp.mean(x * x, axis=-1, keepdims=True) + epsilon)
        normed = (x * scale * gain_ref[...]).astype(jnp.bfloat16)
        out_ref[:, at * count : (at + 1) * count] = normed.T


def normalize_rows(x, other, gain):
    return pl.pallas_call(
        normalize_kernel,
        in_specs=in_vmem(3),
        out_specs=pl.BlockSpec(memory_space=pltpu.VMEM),
        out_shape=jax.ShapeDtypeStruct((x.shape[1], 2 * x.shape[0]), jnp.bfloat16),
        compiler_params=pltpu.CompilerParams(vmem_limit_bytes=20 << 20),
        name="normalize_rows",
    )(x, other, gain)


def project_kernel(normed_ref, *refs):
    *slab_refs, own_ref, sent_ref = refs
    count = own_ref.shape[1]
    rows = slab_refs[0].shape[0]
    for at, slab_ref in enumerate(slab_refs):
        part = jnp.dot(
            slab_ref[...], normed_ref[...], preferred_element_type=jnp.float32
        ).astype(jnp.bfloat16)
        own_ref[at * rows : (at + 1) * rows, :] = part[:, :count]
        sent_ref[at * rows : (at + 1) * rows, :] = part[:, count:]


def project(normed, slabs):
    count = normed.shape[1] // 2
    shape = jax.ShapeDtypeStruct((len(slabs) * slabs[0].shape[0], count), jnp.bfloat16)
    return pl.pallas_call(
        project_kernel,
        in_specs=in_vmem(1 + len(slabs)),
        out_specs=in_vmem(2),
        out_shape=[shape, shape],
        compiler_params=pltpu.CompilerParams(vmem_limit_bytes=20 << 20),
        name="project",
    )(normed, *slabs)


def attention_kernel(first_ref, *refs, pieces, head_width, rows):
    piece_refs = refs[:pieces]
    key_ref, query_ref, out_ref, qkv_ref, context_ref, sems = refs[pieces:]
    width = out_ref.shape[1]

    @pl.when(pl.program_id(0) == 0)
    def _():
        copies = []
        for piece_ref in piece_refs:
            for at in range(0, piece_ref.shape[0], rows):
                number = len(copies)
                first = pl.multiple_of(first_ref[number], rows)
                copies.append(
                    pltpu.make_async_copy(
                        piece_ref.at[at : at + rows, :],
                        qkv_ref.at[pl.ds(first, rows), :],
                        sems.at[number],
                    )
                )
                copies[-1].start()
        for copy in copies:
            copy.wait()

    unit = pl.program_id(0)
    patches = pl.ds(pl.multiple_of(unit * UNIT, UNIT), UNIT)
    query_id = query_ref[pl.ds(unit, 1), :]
    allowed = key_ref[...] == query_id
    for head in range(width // head_width):
        query, key, value = (
            qkv_ref[part * width + head * head_width : part * width + (head + 1) * head_width, patches]
            for part in range(3)
        )
        scores = lax.dot_general(
            key, query, (((0,), (0,)), ((), ())), preferred_element_type=jnp.float32
        )
        scores = jnp.where(allowed, scores, -1e30)
        highest = jnp.max(scores, axis=0, keepdims=True)
        weights = jnp.exp2((scores - highest) * (1.0 / (math.sqrt(head_width) * math.log(2.0))))
        total = jnp.sum(weights, axis=0, keepdims=True)
        weights = weights * jnp.where(query_id >= 0, 1.0 / total, 0.0)
        context_ref[head * head_width : (head + 1) * head_width, :] = jnp.dot(
            value, weights.astype(jnp.bfloat16), preferred_element_type=jnp.float32
        ).astype(jnp.bfloat16)
    out_ref[...] = context_ref[...].T


def attention(pieces, rows, key_id, query_id):
    firsts, *pieces = pieces
    units, count = query_id.shape[0], pieces[0].shape[1]
    total = sum(piece.shape[0] for piece in pieces)
    width = total // 3
    return pl.pallas_call(
        lambda *refs: attention_kernel(
            *refs, pieces=len(pieces), head_width=width // HEADS, rows=rows
        ),
        grid=(units,),
        in_specs=[pl.BlockSpec(memory_space=pltpu.SMEM)]
        + [pl.BlockSpec(memory_space=pltpu.HBM)] * len(pieces)
        + [
            pl.BlockSpec((UNIT, 1), lambda n: (n, 0)),
            pl.BlockSpec((units, UNIT), lambda n: (0, 0)),
        ],
        out_specs=pl.BlockSpec((UNIT, width), lambda n: (n, 0)),
        out_shape=jax.ShapeDtypeStruct((count, width), jnp.bfloat16),
        scratch_shapes=[
            pltpu.VMEM((total, count), jnp.bfloat16),
            pltpu.VMEM((width, UNIT), jnp.bfloat16),
            pltpu.SemaphoreType.DMA((total // rows,)),
        ],
        compiler_params=pltpu.CompilerParams(
            dimension_semantics=("arbitrary",), vmem_limit_bytes=20 << 20
        ),
        name="attention",
    )(firsts, *(in_hbm(piece) for piece in pieces), key_id, query_id)


def merge_kernel(
    core_ref, context_ref, w_own_ref, w_other_ref, x_ref, gain_ref, out_ref, hidden_ref, merged_ref
):
    core = core_ref[0]
    count, width = context_ref.shape
    half = width // 2
    for w_ref, place in ((w_own_ref, core), (w_other_ref, 1 - core)):
        hidden_ref[place] = jnp.dot(
            context_ref[...], w_ref[...], preferred_element_type=jnp.float32
        )
    low = x_ref[:, :half].astype(jnp.float32) + hidden_ref[0]
    high = x_ref[:, half:].astype(jnp.float32) + hidden_ref[1]
    square = jnp.sum(low * low, axis=-1, keepdims=True) + jnp.sum(
        high * high, axis=-1, keepdims=True
    )
    scale = lax.rsqrt(square * (1.0 / width) + epsilon)
    merged_ref[:, :half] = (low * scale * gain_ref[:, :half]).astype(jnp.bfloat16)
    merged_ref[:, half:] = (high * scale * gain_ref[:, half:]).astype(jnp.bfloat16)
    tokens = out_ref.shape[0]
    units = count // UNIT
    to_row = lax.broadcasted_iota(jnp.int32, (tokens, count), 0)
    from_row = lax.broadcasted_iota(jnp.int32, (tokens, count), 1)
    first_row = (to_row % units) * UNIT + (to_row // units) * 4
    for member in range(4):
        choice = (from_row == first_row + member).astype(jnp.bfloat16)
        out_ref[:, member * width : (member + 1) * width] = jnp.dot(
            choice, merged_ref[...], preferred_element_type=jnp.float32
        ).astype(jnp.bfloat16)


def merge_tokens(core, context, w_own, w_other, x, gain):
    count, width = x.shape
    return pl.pallas_call(
        merge_kernel,
        in_specs=[pl.BlockSpec(memory_space=pltpu.SMEM)] + in_vmem(5),
        out_specs=pl.BlockSpec(memory_space=pltpu.VMEM),
        out_shape=jax.ShapeDtypeStruct((count // 4, 4 * width), jnp.bfloat16),
        scratch_shapes=[
            pltpu.VMEM((2, count, width // 2), jnp.float32),
            pltpu.VMEM((count, width), jnp.bfloat16),
        ],
        compiler_params=pltpu.CompilerParams(vmem_limit_bytes=28 << 20),
        name="merge_tokens",
    )(core, context, on_chip(w_own), on_chip(w_other), x, gain)


def destination_rows(units, samples):
    slots = units.shape[1]
    samples = samples.reshape(-1)
    flat = units.reshape(-1)
    order = jnp.arange(flat.shape[0], dtype=jnp.int32)
    ahead = (samples[:, None] < samples[None, :]) | (
        (samples[:, None] == samples[None, :]) & (order[:, None] < order[None, :])
    )
    starts = jnp.sum(jnp.where(ahead, flat[:, None], 0), axis=0).reshape(units.shape)
    slot = jnp.arange(slots, dtype=jnp.int32)
    offsets = jnp.sum(jnp.where(slot[:, None] < slot[None, :], units[:, :, None], 0), axis=1)
    unit = slot[None, None, :]
    inside = (unit >= offsets[:, :, None]) & (unit < (offsets + units)[:, :, None])
    row = jnp.sum(jnp.where(inside, (starts - offsets)[:, :, None] + unit, 0), axis=1)
    return jnp.where(jnp.any(inside, axis=1), row, -1)


def body(patches, attn_gain, w_qkv, w_out, merge_gain, window_ids, image_patches, image_sample):
    patch_count, width = patches.shape
    token_count = patch_count // 4
    group_size = lax.axis_size("tensor")
    core = (lax.axis_index("pipe") % 2).astype(jnp.int32).reshape(1)

    slots = image_patches.shape[0]
    row_count, qkv_part = w_qkv.shape

    info = jnp.concatenate([image_patches // UNIT, image_sample]).astype(jnp.bfloat16)
    info = jnp.broadcast_to(info[None], (row_count, 2 * slots))
    rows = copy_for_each(jnp.concatenate([w_qkv, info], axis=1), "tensor")
    slab = rows[:, :, :qkv_part].reshape(width, qkv_part).T
    info = rows[:, 0, qkv_part:].astype(jnp.int32)
    dest_rows = destination_rows(info[:, :slots], info[:, slots:])

    slab, w_out = lax.optimization_barrier((slab, w_out))
    live = jnp.arange(patch_count, dtype=jnp.int32) < jnp.sum(image_patches)
    key_id = jnp.where(live, window_ids, -1)[:, None]
    query_id = jnp.where(live, window_ids, -2).reshape(patch_count // UNIT, UNIT)
    pieces, out_own, (key_id, query_id, dest_rows) = ring_project(
        slab, patches, attn_gain[None, :], w_out, core, (key_id, query_id, dest_rows)
    )
    out_other = partner_copy(out_own)
    context = attention(pieces, qkv_part, key_id, query_id)
    tokens = merge_tokens(core, context, out_own, out_other, patches, merge_gain[None, :])
    outgoing = tokens.reshape(group_size, token_count // group_size, 4 * width)
    received = lax.all_to_all(outgoing, "tensor", split_axis=0, concat_axis=0, tiled=True)
    placement = (
        jnp.arange(token_count, dtype=jnp.int32)[:, None] == dest_rows.reshape(1, token_count)
    ).astype(jnp.bfloat16)
    placed = jnp.dot(
        placement, received.reshape(token_count, 4 * width), preferred_element_type=jnp.float32
    )
    return placed.astype(jnp.bfloat16).reshape(1, token_count, 1, 4 * width)


def solution(mesh):
    return jax.shard_map(
        body,
        mesh=mesh,
        in_specs=(
            P(("pipe", "tensor"), None),
            P(),
            P("tensor", "pipe"),
            P("tensor", "pipe"),
            P(),
            P(("pipe", "tensor")),
            P(("pipe", "tensor")),
            P(("pipe", "tensor")),
        ),
        out_specs=P("pipe", None, "tensor", None),
        check_vma=False,
    )
```

```python
import math

import jax
import jax.numpy as jnp
from jax import lax
from jax.experimental import pallas as pl
from jax.experimental.pallas import tpu as pltpu
from jax.sharding import PartitionSpec as P

HEADS = 16
UNIT = 128

epsilon = 1e-06


def copy_for_each(x, axis):
    size = lax.axis_size(axis)
    return lax.all_to_all(jnp.broadcast_to(x[None], (size, *x.shape)), axis, 0, 0, tiled=True)


def partner_copy(x):
    size = lax.axis_size("pipe")
    return lax.ppermute(x, "pipe", [(p, p ^ 1) for p in range(size)])


def in_hbm(x):
    return pltpu.with_memory_space_constraint(x, pltpu.HBM)


def in_vmem(count):
    return [pl.BlockSpec(memory_space=pltpu.VMEM)] * count


def payload_kernel(patches_ref, sample_ref, w_ref, out_ref, wide_ref):
    copies, rows, lanes = out_ref.shape
    columns = w_ref.shape[1]
    slots = patches_ref.shape[0]
    last = lanes - 128
    wide_ref[:, :columns] = w_ref[...].astype(jnp.float32)
    lane = lax.broadcasted_iota(jnp.int32, (rows, 128), 1) + last
    tail = jnp.where(lane < columns, wide_ref[:, last:], 0.0)
    for slot in range(slots):
        units = (patches_ref[slot] // UNIT).astype(jnp.float32)
        tail = jnp.where(lane == columns + slot, units, tail)
        sample = sample_ref[slot].astype(jnp.float32)
        tail = jnp.where(lane == columns + slots + slot, sample, tail)
    head = wide_ref[:, :last].astype(jnp.bfloat16)
    tail = tail.astype(jnp.bfloat16)
    for copy in range(copies):
        out_ref[copy, :, :last] = head
        out_ref[copy, :, last:] = tail


def payload_copies(image_patches, image_sample, w, copies):
    rows, columns = w.shape
    lanes = -(-(columns + 2 * image_patches.shape[0]) // 128) * 128
    return pl.pallas_call(
        payload_kernel,
        in_specs=[pl.BlockSpec(memory_space=pltpu.SMEM)] * 2 + in_vmem(1),
        out_specs=pl.BlockSpec(memory_space=pltpu.VMEM),
        out_shape=jax.ShapeDtypeStruct((copies, rows, lanes), jnp.bfloat16),
        scratch_shapes=[pltpu.VMEM((rows, lanes), jnp.float32)],
        compiler_params=pltpu.CompilerParams(vmem_limit_bytes=8 << 20),
        name="payload_copies",
    )(image_patches, image_sample, w)


def normalize_kernel(x_ref, gain_ref, out_ref):
    x = x_ref[...].astype(jnp.float32)
    scale = lax.rsqrt(jnp.mean(x * x, axis=-1, keepdims=True) + epsilon)
    out_ref[...] = (x * scale * gain_ref[...]).astype(jnp.bfloat16).T


def normalize_rows(x, gain):
    return pl.pallas_call(
        normalize_kernel,
        in_specs=in_vmem(2),
        out_specs=pl.BlockSpec(memory_space=pltpu.VMEM),
        out_shape=jax.ShapeDtypeStruct((x.shape[1], x.shape[0]), jnp.bfloat16),
        compiler_params=pltpu.CompilerParams(vmem_limit_bytes=16 << 20),
        name="normalize_rows",
    )(x, gain)


def project_kernel(w_ref, normed_ref, out_ref):
    out_ref[...] = jnp.dot(
        w_ref[...], normed_ref[...], preferred_element_type=jnp.float32
    ).astype(jnp.bfloat16)


def project(w, normed):
    width, count = normed.shape
    chunk = 3 * width // 4
    return pl.pallas_call(
        project_kernel,
        grid=(4,),
        in_specs=[
            pl.BlockSpec((chunk, width), lambda n: (n, 0)),
            pl.BlockSpec((width, count), lambda n: (0, 0)),
        ],
        out_specs=pl.BlockSpec((chunk, count), lambda n: (n, 0)),
        out_shape=pltpu.HBM((3 * width, count), jnp.bfloat16),
        compiler_params=pltpu.CompilerParams(
            dimension_semantics=("arbitrary",), vmem_limit_bytes=20 << 20
        ),
        name="project",
    )(in_hbm(w), normed)


def attention_kernel(qkv_ref, key_ref, query_ref, out_ref, context_ref, *, head_width):
    width = out_ref.shape[1]
    query_id = query_ref[pl.ds(pl.program_id(0), 1), :]
    allowed = key_ref[...] == query_id
    for head in range(width // head_width):
        query, key, value = (
            qkv_ref[part * width + head * head_width : part * width + (head + 1) * head_width, :]
            for part in range(3)
        )
        scores = lax.dot_general(
            key, query, (((0,), (0,)), ((), ())), preferred_element_type=jnp.float32
        )
        scores = jnp.where(allowed, scores, -1e30)
        highest = jnp.max(scores, axis=0, keepdims=True)
        weights = jnp.exp2((scores - highest) * (1.0 / (math.sqrt(head_width) * math.log(2.0))))
        total = jnp.sum(weights, axis=0, keepdims=True)
        weights = weights * jnp.where(query_id >= 0, 1.0 / total, 0.0)
        context_ref[head * head_width : (head + 1) * head_width, :] = jnp.dot(
            value, weights.astype(jnp.bfloat16), preferred_element_type=jnp.float32
        ).astype(jnp.bfloat16)
    out_ref[...] = context_ref[...].T


def attention(qkv, key_id, query_id):
    width, count = qkv.shape[0] // 3, qkv.shape[1]
    units = count // UNIT
    return pl.pallas_call(
        lambda *refs: attention_kernel(*refs, head_width=width // HEADS),
        grid=(units,),
        in_specs=[
            pl.BlockSpec((3 * width, UNIT), lambda n: (0, n)),
            pl.BlockSpec((UNIT, 1), lambda n: (n, 0)),
            pl.BlockSpec((units, UNIT), lambda n: (0, 0)),
        ],
        out_specs=pl.BlockSpec((UNIT, width), lambda n: (n, 0)),
        out_shape=jax.ShapeDtypeStruct((count, width), jnp.bfloat16),
        scratch_shapes=[pltpu.VMEM((width, UNIT), jnp.bfloat16)],
        compiler_params=pltpu.CompilerParams(
            dimension_semantics=("arbitrary",), vmem_limit_bytes=16 << 20
        ),
        name="attention",
    )(in_hbm(qkv), key_id, query_id)


def merge_kernel(
    core_ref, context_ref, w_own_ref, w_other_ref, x_ref, gain_ref, out_ref, hidden_ref, merged_ref
):
    core = core_ref[0]
    count, width = context_ref.shape
    half = width // 2
    for w_ref, place in ((w_own_ref, core), (w_other_ref, 1 - core)):
        hidden_ref[place] = jnp.dot(
            context_ref[...], w_ref[...], preferred_element_type=jnp.float32
        )
    low = x_ref[:, :half].astype(jnp.float32) + hidden_ref[0]
    high = x_ref[:, half:].astype(jnp.float32) + hidden_ref[1]
    square = jnp.sum(low * low, axis=-1, keepdims=True) + jnp.sum(
        high * high, axis=-1, keepdims=True
    )
    scale = lax.rsqrt(square * (1.0 / width) + epsilon)
    merged_ref[:, :half] = (low * scale * gain_ref[:, :half]).astype(jnp.bfloat16)
    merged_ref[:, half:] = (high * scale * gain_ref[:, half:]).astype(jnp.bfloat16)
    tokens = out_ref.shape[0]
    units = count // UNIT
    to_row = lax.broadcasted_iota(jnp.int32, (tokens, count), 0)
    from_row = lax.broadcasted_iota(jnp.int32, (tokens, count), 1)
    first_row = (to_row % units) * UNIT + (to_row // units) * 4
    for member in range(4):
        choice = (from_row == first_row + member).astype(jnp.bfloat16)
        out_ref[:, member * width : (member + 1) * width] = jnp.dot(
            choice, merged_ref[...], preferred_element_type=jnp.float32
        ).astype(jnp.bfloat16)


def merge_tokens(core, context, w_own, w_other, x, gain):
    count, width = x.shape
    return pl.pallas_call(
        merge_kernel,
        in_specs=[pl.BlockSpec(memory_space=pltpu.SMEM)] + in_vmem(5),
        out_specs=pl.BlockSpec(memory_space=pltpu.VMEM),
        out_shape=jax.ShapeDtypeStruct((count // 4, 4 * width), jnp.bfloat16),
        scratch_shapes=[
            pltpu.VMEM((2, count, width // 2), jnp.float32),
            pltpu.VMEM((count, width), jnp.bfloat16),
        ],
        compiler_params=pltpu.CompilerParams(vmem_limit_bytes=28 << 20),
        name="merge_tokens",
    )(core, context, w_own, in_hbm(w_other), x, gain)


def destination_rows(units, samples):
    slots = units.shape[1]
    samples = samples.reshape(-1)
    flat = units.reshape(-1)
    order = jnp.arange(flat.shape[0], dtype=jnp.int32)
    ahead = (samples[:, None] < samples[None, :]) | (
        (samples[:, None] == samples[None, :]) & (order[:, None] < order[None, :])
    )
    starts = jnp.sum(jnp.where(ahead, flat[:, None], 0), axis=0).reshape(units.shape)
    slot = jnp.arange(slots, dtype=jnp.int32)
    offsets = jnp.sum(jnp.where(slot[:, None] < slot[None, :], units[:, :, None], 0), axis=1)
    unit = slot[None, None, :]
    inside = (unit >= offsets[:, :, None]) & (unit < (offsets + units)[:, :, None])
    row = jnp.sum(jnp.where(inside, (starts - offsets)[:, :, None] + unit, 0), axis=1)
    return jnp.where(jnp.any(inside, axis=1), row, -1)


def body(patches, attn_gain, w_qkv, w_out, merge_gain, window_ids, image_patches, image_sample):
    patch_count, width = patches.shape
    token_count = patch_count // 4
    group_size = lax.axis_size("tensor")
    core = (lax.axis_index("pipe") % 2).astype(jnp.int32).reshape(1)

    half = width // 2
    slots = image_patches.shape[0]
    row_count, qkv_part = w_qkv.shape

    together = lax.optimization_barrier
    payload = payload_copies(image_patches, image_sample, w_qkv, group_size)
    rows = lax.all_to_all(payload, "tensor", 0, 0, tiled=True)
    slab = rows[:, :, :qkv_part].reshape(width, qkv_part).T
    w_all = lax.all_gather(slab, "pipe", axis=0, tiled=True)
    info = rows[:, 0, qkv_part : qkv_part + 2 * slots].astype(jnp.int32)

    slab, w_out, patches = together((slab, w_out, patches))
    normed = normalize_rows(patches, attn_gain[None, :])
    live = jnp.arange(patch_count, dtype=jnp.int32) < jnp.sum(image_patches)
    key_id = jnp.where(live, window_ids, -1)[:, None]
    query_id = jnp.where(live, window_ids, -2).reshape(patch_count // UNIT, UNIT)
    blocks = copy_for_each(w_out, "pipe")
    blocks, normed, key_id, query_id = together((blocks, normed, key_id, query_id))
    out_rows = jnp.moveaxis(blocks, 0, 1).reshape(row_count, 2, half)
    out_rows = lax.dynamic_index_in_dim(out_rows, core[0], axis=1, keepdims=False)
    out_own = copy_for_each(out_rows, "tensor")
    qkv = project(w_all, normed)
    qkv, out_own = together((qkv, out_own))
    out_own = out_own.reshape(width, half)
    out_other = partner_copy(out_own)
    context = attention(qkv, key_id, query_id)
    tokens = merge_tokens(core, context, out_own, out_other, patches, merge_gain[None, :])
    tokens, info = together((tokens, info))
    dest_rows = destination_rows(info[:, :slots], info[:, slots:])
    outgoing = tokens.reshape(group_size, token_count // group_size, 4 * width)
    received = lax.all_to_all(outgoing, "tensor", split_axis=0, concat_axis=0, tiled=True)
    placement = (
        jnp.arange(token_count, dtype=jnp.int32)[:, None] == dest_rows.reshape(1, token_count)
    ).astype(jnp.bfloat16)
    placed = jnp.dot(
        placement, received.reshape(token_count, 4 * width), preferred_element_type=jnp.float32
    )
    return placed.astype(jnp.bfloat16).reshape(1, token_count, 1, 4 * width)


def solution(mesh):
    return jax.shard_map(
        body,
        mesh=mesh,
        in_specs=(
            P(("pipe", "tensor"), None),
            P(),
            P("tensor", "pipe"),
            P("tensor", "pipe"),
            P(),
            P(("pipe", "tensor")),
            P(("pipe", "tensor")),
            P(("pipe", "tensor")),
        ),
        out_specs=P("pipe", None, "tensor", None),
        check_vma=False,
    )
```

```python
import math

import jax
import jax.numpy as jnp
from jax import lax
from jax.experimental import pallas as pl
from jax.experimental.pallas import tpu as pltpu
from jax.sharding import PartitionSpec as P

HEADS = 16
UNIT = 128

epsilon = 1e-06


def copy_for_each(x, axis):
    size = lax.axis_size(axis)
    return lax.all_to_all(jnp.broadcast_to(x[None], (size, *x.shape)), axis, 0, 0, tiled=True)


def partner_copy(x):
    size = lax.axis_size("pipe")
    return lax.ppermute(x, "pipe", [(p, p ^ 1) for p in range(size)])


def in_hbm(x):
    return pltpu.with_memory_space_constraint(x, pltpu.HBM)


def in_vmem(count):
    return [pl.BlockSpec(memory_space=pltpu.VMEM)] * count


def payload_kernel(patches_ref, sample_ref, w_ref, out_ref, wide_ref):
    copies, rows, lanes = out_ref.shape
    columns = w_ref.shape[1]
    slots = patches_ref.shape[0]
    last = lanes - 128
    wide_ref[:, :columns] = w_ref[...].astype(jnp.float32)
    lane = lax.broadcasted_iota(jnp.int32, (rows, 128), 1) + last
    tail = jnp.where(lane < columns, wide_ref[:, last:], 0.0)
    for slot in range(slots):
        units = (patches_ref[slot] // UNIT).astype(jnp.float32)
        tail = jnp.where(lane == columns + slot, units, tail)
        sample = sample_ref[slot].astype(jnp.float32)
        tail = jnp.where(lane == columns + slots + slot, sample, tail)
    head = wide_ref[:, :last].astype(jnp.bfloat16)
    tail = tail.astype(jnp.bfloat16)
    for copy in range(copies):
        out_ref[copy, :, :last] = head
        out_ref[copy, :, last:] = tail


def payload_copies(image_patches, image_sample, w, copies):
    rows, columns = w.shape
    lanes = -(-(columns + 2 * image_patches.shape[0]) // 128) * 128
    return pl.pallas_call(
        payload_kernel,
        in_specs=[pl.BlockSpec(memory_space=pltpu.SMEM)] * 2 + in_vmem(1),
        out_specs=pl.BlockSpec(memory_space=pltpu.VMEM),
        out_shape=jax.ShapeDtypeStruct((copies, rows, lanes), jnp.bfloat16),
        scratch_shapes=[pltpu.VMEM((rows, lanes), jnp.float32)],
        compiler_params=pltpu.CompilerParams(vmem_limit_bytes=8 << 20),
        name="payload_copies",
    )(in_hbm(image_patches), in_hbm(image_sample), in_hbm(w))


def normalize_kernel(x_ref, gain_ref, out_ref):
    x = x_ref[...].astype(jnp.float32)
    scale = lax.rsqrt(jnp.mean(x * x, axis=-1, keepdims=True) + epsilon)
    out_ref[...] = (x * scale * gain_ref[...]).astype(jnp.bfloat16).T


def normalize_rows(x, gain):
    return pl.pallas_call(
        normalize_kernel,
        in_specs=in_vmem(2),
        out_specs=pl.BlockSpec(memory_space=pltpu.VMEM),
        out_shape=jax.ShapeDtypeStruct((x.shape[1], x.shape[0]), jnp.bfloat16),
        compiler_params=pltpu.CompilerParams(vmem_limit_bytes=16 << 20),
        name="normalize_rows",
    )(x, gain)


def attention_kernel(
    normed_ref, w_ref, key_ref, query_ref, out_ref, qkv_ref, context_ref, *, head_width
):
    step = pl.program_id(0)
    chunk, width = w_ref.shape
    chunks = 3 * width // chunk

    @pl.when(step < chunks)
    def _():
        qkv_ref[pl.ds(pl.multiple_of(step * chunk, chunk), chunk), :] = jnp.dot(
            w_ref[...], normed_ref[...], preferred_element_type=jnp.float32
        ).astype(jnp.bfloat16)

    @pl.when(step >= chunks)
    def _():
        unit = step - chunks
        patches = pl.ds(pl.multiple_of(unit * UNIT, UNIT), UNIT)
        query_id = query_ref[pl.ds(unit, 1), :]
        key_id = jnp.broadcast_to(key_ref[pl.ds(unit, 1), :], (UNIT, UNIT)).T
        allowed = key_id == query_id
        heads = range(width // head_width)

        def rows(part, head):
            first = part * width + head * head_width
            return qkv_ref[first : first + head_width, patches]

        scores = [
            lax.dot_general(
                rows(1, head), rows(0, head), (((0,), (0,)), ((), ())), preferred_element_type=jnp.float32
            )
            for head in heads
        ]
        scores = [jnp.where(allowed, score, -1e30) for score in scores]
        highest = [jnp.max(score, axis=0, keepdims=True) for score in scores]
        factor = 1.0 / (math.sqrt(head_width) * math.log(2.0))
        weights = [jnp.exp2((score - top) * factor) for score, top in zip(scores, highest)]
        totals = [jnp.sum(weight, axis=0, keepdims=True) for weight in weights]
        weights = [
            (weight * jnp.where(query_id >= 0, 1.0 / total, 0.0)).astype(jnp.bfloat16)
            for weight, total in zip(weights, totals)
        ]
        for head, weight in zip(heads, weights):
            context_ref[head * head_width : (head + 1) * head_width, :] = jnp.dot(
                rows(2, head), weight, preferred_element_type=jnp.float32
            ).astype(jnp.bfloat16)
        out_ref[...] = context_ref[...].T


def attention(w, normed, key_id, query_id):
    width, count = normed.shape
    chunk = 3 * width // 4
    units = count // UNIT
    whole = lambda *shape: pl.BlockSpec(shape, lambda n: (0,) * len(shape))
    return pl.pallas_call(
        lambda *refs: attention_kernel(*refs, head_width=width // HEADS),
        grid=(4 + units,),
        in_specs=[
            whole(width, count),
            pl.BlockSpec((chunk, width), lambda n: (jnp.minimum(n, 3), 0)),
            whole(units, UNIT),
            whole(units, UNIT),
        ],
        out_specs=pl.BlockSpec((UNIT, width), lambda n: (jnp.maximum(n - 4, 0), 0)),
        out_shape=jax.ShapeDtypeStruct((count, width), jnp.bfloat16),
        scratch_shapes=[
            pltpu.VMEM((3 * width, count), jnp.bfloat16),
            pltpu.VMEM((width, UNIT), jnp.bfloat16),
        ],
        compiler_params=pltpu.CompilerParams(
            dimension_semantics=("arbitrary",), vmem_limit_bytes=32 << 20
        ),
        name="attention",
    )(normed, in_hbm(w), key_id, query_id)


def merge_kernel(
    core_ref, context_ref, w_own_ref, w_other_ref, x_ref, gain_ref, out_ref, hidden_ref, merged_ref
):
    core = core_ref[0]
    count, width = context_ref.shape
    half = width // 2
    for w_ref, place in ((w_own_ref, core), (w_other_ref, 1 - core)):
        hidden_ref[place] = jnp.dot(
            context_ref[...], w_ref[...], preferred_element_type=jnp.float32
        )
    low = x_ref[:, :half].astype(jnp.float32) + hidden_ref[0]
    high = x_ref[:, half:].astype(jnp.float32) + hidden_ref[1]
    square = jnp.sum(low * low, axis=-1, keepdims=True) + jnp.sum(
        high * high, axis=-1, keepdims=True
    )
    scale = lax.rsqrt(square * (1.0 / width) + epsilon)
    merged_ref[:, :half] = (low * scale * gain_ref[:, :half]).astype(jnp.bfloat16)
    merged_ref[:, half:] = (high * scale * gain_ref[:, half:]).astype(jnp.bfloat16)
    tokens = out_ref.shape[0] * out_ref.shape[1]
    units = count // UNIT
    to_row = lax.broadcasted_iota(jnp.int32, (tokens, count), 0)
    from_row = lax.broadcasted_iota(jnp.int32, (tokens, count), 1)
    first_row = (to_row % units) * UNIT + (to_row // units) * 4
    for member in range(4):
        choice = (from_row == first_row + member).astype(jnp.bfloat16)
        part = jnp.dot(choice, merged_ref[...], preferred_element_type=jnp.float32)
        out_ref[:, :, member * width : (member + 1) * width] = part.reshape(
            -1, units, width
        ).astype(jnp.bfloat16)


def merge_tokens(core, context, w_own, w_other, x, gain):
    count, width = x.shape
    return pl.pallas_call(
        merge_kernel,
        in_specs=[pl.BlockSpec(memory_space=pltpu.SMEM)] + in_vmem(5),
        out_specs=pl.BlockSpec(memory_space=pltpu.VMEM),
        out_shape=jax.ShapeDtypeStruct((UNIT // 4, count // UNIT, 4 * width), jnp.bfloat16),
        scratch_shapes=[
            pltpu.VMEM((2, count, width // 2), jnp.float32),
            pltpu.VMEM((count, width), jnp.bfloat16),
        ],
        compiler_params=pltpu.CompilerParams(vmem_limit_bytes=28 << 20),
        name="merge_tokens",
    )(core, context, w_own, in_hbm(w_other), x, gain)


def destination_rows(units, samples):
    slots = units.shape[1]
    samples = samples.reshape(-1)
    flat = units.reshape(-1)
    order = jnp.arange(flat.shape[0], dtype=jnp.int32)
    ahead = (samples[:, None] < samples[None, :]) | (
        (samples[:, None] == samples[None, :]) & (order[:, None] < order[None, :])
    )
    starts = jnp.sum(jnp.where(ahead, flat[:, None], 0), axis=0).reshape(units.shape)
    slot = jnp.arange(slots, dtype=jnp.int32)
    offsets = jnp.sum(jnp.where(slot[:, None] < slot[None, :], units[:, :, None], 0), axis=1)
    unit = slot[None, None, :]
    inside = (unit >= offsets[:, :, None]) & (unit < (offsets + units)[:, :, None])
    row = jnp.sum(jnp.where(inside, (starts - offsets)[:, :, None] + unit, 0), axis=1)
    return jnp.where(jnp.any(inside, axis=1), row, -1)


def body(patches, attn_gain, w_qkv, w_out, merge_gain, window_ids, image_patches, image_sample):
    patch_count, width = patches.shape
    token_count = patch_count // 4
    group_size = lax.axis_size("tensor")
    core = (lax.axis_index("pipe") % 2).astype(jnp.int32).reshape(1)

    half = width // 2
    slots = image_patches.shape[0]
    row_count, qkv_part = w_qkv.shape

    together = lax.optimization_barrier
    payload = payload_copies(image_patches, image_sample, w_qkv, group_size)
    rows = lax.all_to_all(payload, "tensor", 0, 0, tiled=True)
    slab = rows[:, :, :qkv_part].reshape(width, qkv_part).T
    w_all = lax.all_gather(slab, "pipe", axis=0, tiled=True)

    slab, w_out, patches = together((slab, w_out, patches))
    blocks = copy_for_each(w_out, "pipe")
    normed = normalize_rows(patches, attn_gain[None, :])
    live = jnp.arange(patch_count, dtype=jnp.int32) < jnp.sum(image_patches)
    key_id = jnp.where(live, window_ids, -1).reshape(patch_count // UNIT, UNIT)
    query_id = jnp.where(live, window_ids, -2).reshape(patch_count // UNIT, UNIT)
    info = rows[:, 0, qkv_part : qkv_part + 2 * slots].astype(jnp.int32)
    merge_row = merge_gain[None, :]
    blocks, normed, key_id, query_id, info, merge_row = together(
        (blocks, normed, key_id, query_id, info, merge_row)
    )
    out_rows = jnp.moveaxis(blocks, 0, 1).reshape(row_count, 2, half)
    out_rows = lax.dynamic_index_in_dim(out_rows, core[0], axis=1, keepdims=False)
    out_own = copy_for_each(out_rows, "tensor").reshape(width, half)
    out_other = partner_copy(out_own)
    context = attention(w_all, normed, key_id, query_id)
    tokens = merge_tokens(core, context, out_own, out_other, patches, merge_row)
    tokens, info = together((tokens, info))
    dest_rows = destination_rows(info[:, :slots], info[:, slots:])
    received = lax.all_to_all(tokens, "tensor", split_axis=0, concat_axis=0, tiled=True)
    placement = (
        jnp.arange(token_count, dtype=jnp.int32)[:, None] == dest_rows.reshape(1, token_count)
    ).astype(jnp.bfloat16)
    placed = jnp.dot(
        placement, received.reshape(token_count, 4 * width), preferred_element_type=jnp.float32
    )
    return placed.astype(jnp.bfloat16).reshape(1, token_count, 1, 4 * width)


def solution(mesh):
    return jax.shard_map(
        body,
        mesh=mesh,
        in_specs=(
            P(("pipe", "tensor"), None),
            P(),
            P("tensor", "pipe"),
            P("tensor", "pipe"),
            P(),
            P(("pipe", "tensor")),
            P(("pipe", "tensor")),
            P(("pipe", "tensor")),
        ),
        out_specs=P("pipe", None, "tensor", None),
        check_vma=False,
    )
```

```python
import math

import jax
import jax.numpy as jnp
from jax import lax
from jax.experimental import pallas as pl
from jax.experimental.pallas import tpu as pltpu
from jax.sharding import PartitionSpec as P

HEADS = 16
UNIT = 128

epsilon = 1e-06


def copy_for_each(x, axis):
    size = lax.axis_size(axis)
    return lax.all_to_all(jnp.broadcast_to(x[None], (size, *x.shape)), axis, 0, 0, tiled=True)


def partner_copy(x):
    size = lax.axis_size("pipe")
    return lax.ppermute(x, "pipe", [(p, p ^ 1) for p in range(size)])


def in_hbm(x):
    return pltpu.with_memory_space_constraint(x, pltpu.HBM)


def in_vmem(count):
    return [pl.BlockSpec(memory_space=pltpu.VMEM)] * count


def payload_kernel(patches_ref, sample_ref, w_ref, out_ref, wide_ref):
    copies, rows, lanes = out_ref.shape
    columns = w_ref.shape[1]
    slots = patches_ref.shape[0]
    last = lanes - 128
    wide_ref[:, :columns] = w_ref[...].astype(jnp.float32)
    lane = lax.broadcasted_iota(jnp.int32, (rows, 128), 1) + last
    tail = jnp.where(lane < columns, wide_ref[:, last:], 0.0)
    for slot in range(slots):
        units = (patches_ref[slot] // UNIT).astype(jnp.float32)
        tail = jnp.where(lane == columns + slot, units, tail)
        sample = sample_ref[slot].astype(jnp.float32)
        tail = jnp.where(lane == columns + slots + slot, sample, tail)
    head = wide_ref[:, :last].astype(jnp.bfloat16)
    tail = tail.astype(jnp.bfloat16)
    for copy in range(copies):
        out_ref[copy, :, :last] = head
        out_ref[copy, :, last:] = tail


def payload_copies(image_patches, image_sample, w, copies):
    rows, columns = w.shape
    lanes = -(-(columns + 2 * image_patches.shape[0]) // 128) * 128
    return pl.pallas_call(
        payload_kernel,
        in_specs=[pl.BlockSpec(memory_space=pltpu.SMEM)] * 2 + in_vmem(1),
        out_specs=pl.BlockSpec(memory_space=pltpu.VMEM),
        out_shape=jax.ShapeDtypeStruct((copies, rows, lanes), jnp.bfloat16),
        scratch_shapes=[pltpu.VMEM((rows, lanes), jnp.float32)],
        compiler_params=pltpu.CompilerParams(vmem_limit_bytes=8 << 20),
        name="payload_copies",
    )(in_hbm(image_patches), in_hbm(image_sample), in_hbm(w))


def normalize_kernel(x_ref, gain_ref, out_ref):
    x = x_ref[...].astype(jnp.float32)
    scale = lax.rsqrt(jnp.mean(x * x, axis=-1, keepdims=True) + epsilon)
    out_ref[...] = (x * scale * gain_ref[...]).astype(jnp.bfloat16).T


def normalize_rows(x, gain):
    return pl.pallas_call(
        normalize_kernel,
        in_specs=in_vmem(2),
        out_specs=pl.BlockSpec(memory_space=pltpu.VMEM),
        out_shape=jax.ShapeDtypeStruct((x.shape[1], x.shape[0]), jnp.bfloat16),
        compiler_params=pltpu.CompilerParams(vmem_limit_bytes=16 << 20),
        name="normalize_rows",
    )(x, gain)


def attention_kernel(
    normed_ref, w_ref, key_ref, query_ref, out_ref, qkv_ref, context_ref, *, head_width
):
    step = pl.program_id(0)
    chunk, width = w_ref.shape
    chunks = 3 * width // chunk

    @pl.when(step < chunks)
    def _():
        qkv_ref[pl.ds(pl.multiple_of(step * chunk, chunk), chunk), :] = jnp.dot(
            w_ref[...], normed_ref[...], preferred_element_type=jnp.float32
        ).astype(jnp.bfloat16)

    @pl.when(step >= chunks)
    def _():
        unit = step - chunks
        patches = pl.ds(pl.multiple_of(unit * UNIT, UNIT), UNIT)
        query_id = query_ref[pl.ds(unit, 1), :]
        key_id = jnp.broadcast_to(key_ref[pl.ds(unit, 1), :], (UNIT, UNIT)).T
        allowed = key_id == query_id
        heads = range(width // head_width)

        def rows(part, head):
            first = part * width + head * head_width
            return qkv_ref[first : first + head_width, patches]

        scores = [
            lax.dot_general(
                rows(1, head), rows(0, head), (((0,), (0,)), ((), ())), preferred_element_type=jnp.float32
            )
            for head in heads
        ]
        scores = [jnp.where(allowed, score, -1e30) for score in scores]
        highest = [jnp.max(score, axis=0, keepdims=True) for score in scores]
        factor = 1.0 / (math.sqrt(head_width) * math.log(2.0))
        weights = [jnp.exp2((score - top) * factor) for score, top in zip(scores, highest)]
        totals = [jnp.sum(weight, axis=0, keepdims=True) for weight in weights]
        weights = [
            (weight * jnp.where(query_id >= 0, 1.0 / total, 0.0)).astype(jnp.bfloat16)
            for weight, total in zip(weights, totals)
        ]
        for head, weight in zip(heads, weights):
            context_ref[head * head_width : (head + 1) * head_width, :] = jnp.dot(
                rows(2, head), weight, preferred_element_type=jnp.float32
            ).astype(jnp.bfloat16)
        out_ref[...] = context_ref[...].T


def attention(w, normed, key_id, query_id):
    width, count = normed.shape
    chunk = 3 * width // 4
    units = count // UNIT
    whole = lambda *shape: pl.BlockSpec(shape, lambda n: (0,) * len(shape))
    return pl.pallas_call(
        lambda *refs: attention_kernel(*refs, head_width=width // HEADS),
        grid=(4 + units,),
        in_specs=[
            whole(width, count),
            pl.BlockSpec((chunk, width), lambda n: (jnp.minimum(n, 3), 0)),
            whole(units, UNIT),
            whole(units, UNIT),
        ],
        out_specs=pl.BlockSpec((UNIT, width), lambda n: (jnp.maximum(n - 4, 0), 0)),
        out_shape=jax.ShapeDtypeStruct((count, width), jnp.bfloat16),
        scratch_shapes=[
            pltpu.VMEM((3 * width, count), jnp.bfloat16),
            pltpu.VMEM((width, UNIT), jnp.bfloat16),
        ],
        compiler_params=pltpu.CompilerParams(
            dimension_semantics=("arbitrary",), vmem_limit_bytes=32 << 20
        ),
        name="attention",
    )(in_hbm(normed), in_hbm(w), key_id, query_id)


def merge_kernel(
    core_ref, context_ref, w_own_ref, w_other_ref, x_ref, gain_ref, out_ref, hidden_ref, merged_ref, held_ref, sem
):
    core = core_ref[0]
    count, width = context_ref.shape
    half = width // 2
    load = pltpu.make_async_copy(w_other_ref, held_ref, sem)
    load.start()
    hidden_ref[core] = jnp.dot(
        context_ref[...], w_own_ref[...], preferred_element_type=jnp.float32
    )
    load.wait()
    hidden_ref[1 - core] = jnp.dot(
        context_ref[...], held_ref[...], preferred_element_type=jnp.float32
    )
    low = x_ref[:, :half].astype(jnp.float32) + hidden_ref[0]
    high = x_ref[:, half:].astype(jnp.float32) + hidden_ref[1]
    square = jnp.sum(low * low, axis=-1, keepdims=True) + jnp.sum(
        high * high, axis=-1, keepdims=True
    )
    scale = lax.rsqrt(square * (1.0 / width) + epsilon)
    merged_ref[:, :half] = (low * scale * gain_ref[:, :half]).astype(jnp.bfloat16)
    merged_ref[:, half:] = (high * scale * gain_ref[:, half:]).astype(jnp.bfloat16)
    tokens = out_ref.shape[0] * out_ref.shape[1]
    units = count // UNIT
    to_row = lax.broadcasted_iota(jnp.int32, (tokens, count), 0)
    from_row = lax.broadcasted_iota(jnp.int32, (tokens, count), 1)
    first_row = (to_row % units) * UNIT + (to_row // units) * 4
    for member in range(4):
        choice = (from_row == first_row + member).astype(jnp.bfloat16)
        part = jnp.dot(choice, merged_ref[...], preferred_element_type=jnp.float32)
        out_ref[:, :, member * width : (member + 1) * width] = part.reshape(
            -1, units, width
        ).astype(jnp.bfloat16)


def merge_tokens(core, context, w_own, w_other, x, gain):
    count, width = x.shape
    return pl.pallas_call(
        merge_kernel,
        in_specs=[pl.BlockSpec(memory_space=pltpu.SMEM)]
        + in_vmem(2)
        + [pl.BlockSpec(memory_space=pltpu.HBM)]
        + in_vmem(2),
        out_specs=pl.BlockSpec(memory_space=pltpu.VMEM),
        out_shape=pltpu.HBM((UNIT // 4, count // UNIT, 4 * width), jnp.bfloat16),
        scratch_shapes=[
            pltpu.VMEM((2, count, width // 2), jnp.float32),
            pltpu.VMEM((count, width), jnp.bfloat16),
            pltpu.VMEM(w_other.shape, jnp.bfloat16),
            pltpu.SemaphoreType.DMA,
        ],
        compiler_params=pltpu.CompilerParams(vmem_limit_bytes=28 << 20),
        name="merge_tokens",
    )(core, context, w_own, in_hbm(w_other), x, gain)


def destination_rows(units, samples):
    slots = units.shape[1]
    samples = samples.reshape(-1)
    flat = units.reshape(-1)
    order = jnp.arange(flat.shape[0], dtype=jnp.int32)
    ahead = (samples[:, None] < samples[None, :]) | (
        (samples[:, None] == samples[None, :]) & (order[:, None] < order[None, :])
    )
    starts = jnp.sum(jnp.where(ahead, flat[:, None], 0), axis=0).reshape(units.shape)
    slot = jnp.arange(slots, dtype=jnp.int32)
    offsets = jnp.sum(jnp.where(slot[:, None] < slot[None, :], units[:, :, None], 0), axis=1)
    unit = slot[None, None, :]
    inside = (unit >= offsets[:, :, None]) & (unit < (offsets + units)[:, :, None])
    row = jnp.sum(jnp.where(inside, (starts - offsets)[:, :, None] + unit, 0), axis=1)
    return jnp.where(jnp.any(inside, axis=1), row, -1)


def body(patches, attn_gain, w_qkv, w_out, merge_gain, window_ids, image_patches, image_sample):
    patch_count, width = patches.shape
    token_count = patch_count // 4
    group_size = lax.axis_size("tensor")
    core = (lax.axis_index("pipe") % 2).astype(jnp.int32).reshape(1)

    half = width // 2
    slots = image_patches.shape[0]
    row_count, qkv_part = w_qkv.shape

    together = lax.optimization_barrier
    payload = payload_copies(image_patches, image_sample, w_qkv, group_size)
    rows = lax.all_to_all(payload, "tensor", 0, 0, tiled=True)
    slab = rows[:, :, :qkv_part].reshape(width, qkv_part).T
    w_all = lax.all_gather(slab, "pipe", axis=0, tiled=True)

    slab, w_out, patches = together((slab, w_out, patches))
    blocks = copy_for_each(w_out, "pipe")
    normed = normalize_rows(patches, attn_gain[None, :])
    live = jnp.arange(patch_count, dtype=jnp.int32) < jnp.sum(image_patches)
    key_id = jnp.where(live, window_ids, -1).reshape(patch_count // UNIT, UNIT)
    query_id = jnp.where(live, window_ids, -2).reshape(patch_count // UNIT, UNIT)
    info = rows[:, 0, qkv_part : qkv_part + 2 * slots].astype(jnp.int32)
    merge_row = merge_gain[None, :]
    blocks, normed, key_id, query_id, info, merge_row = together(
        (blocks, normed, key_id, query_id, info, merge_row)
    )
    out_rows = jnp.moveaxis(blocks, 0, 1).reshape(row_count, 2, half)
    out_rows = lax.dynamic_index_in_dim(out_rows, core[0], axis=1, keepdims=False)
    out_own = copy_for_each(out_rows, "tensor").reshape(width, half)
    out_other = partner_copy(out_own)
    context = attention(w_all, normed, key_id, query_id)
    tokens = merge_tokens(core, context, out_own, out_other, patches, merge_row)
    tokens, info = together((tokens, info))
    dest_rows = destination_rows(info[:, :slots], info[:, slots:])
    received = lax.all_to_all(tokens, "tensor", split_axis=0, concat_axis=0, tiled=True)
    placement = (
        jnp.arange(token_count, dtype=jnp.int32)[:, None] == dest_rows.reshape(1, token_count)
    ).astype(jnp.bfloat16)
    placed = jnp.dot(
        placement, received.reshape(token_count, 4 * width), preferred_element_type=jnp.float32
    )
    return placed.astype(jnp.bfloat16).reshape(1, token_count, 1, 4 * width)


def solution(mesh):
    return jax.shard_map(
        body,
        mesh=mesh,
        in_specs=(
            P(("pipe", "tensor"), None),
            P(),
            P("tensor", "pipe"),
            P("tensor", "pipe"),
            P(),
            P(("pipe", "tensor")),
            P(("pipe", "tensor")),
            P(("pipe", "tensor")),
        ),
        out_specs=P("pipe", None, "tensor", None),
        check_vma=False,
    )
```

```python
import math

import jax
import jax.numpy as jnp
from jax import lax
from jax.experimental import pallas as pl
from jax.experimental.pallas import tpu as pltpu
from jax.sharding import PartitionSpec as P

HEADS = 16
UNIT = 128

epsilon = 1e-06


def copy_for_each(x, axis):
    size = lax.axis_size(axis)
    return lax.all_to_all(jnp.broadcast_to(x[None], (size, *x.shape)), axis, 0, 0, tiled=True)


def partner_copy(x):
    size = lax.axis_size("pipe")
    return lax.ppermute(x, "pipe", [(p, p ^ 1) for p in range(size)])


def in_hbm(x):
    return pltpu.with_memory_space_constraint(x, pltpu.HBM)


def in_vmem(count):
    return [pl.BlockSpec(memory_space=pltpu.VMEM)] * count


def payload_kernel(patches_ref, sample_ref, w_ref, proj_ref, out_ref, proj_out_ref, wide_ref):
    copies, rows, lanes = out_ref.shape
    columns = w_ref.shape[1]
    slots = patches_ref.shape[0]
    last = lanes - 128
    wide_ref[:, :columns] = w_ref[...].astype(jnp.float32)
    lane = lax.broadcasted_iota(jnp.int32, (rows, 128), 1) + last
    tail = jnp.where(lane < columns, wide_ref[:, last:], 0.0)
    for slot in range(slots):
        units = (patches_ref[slot] // UNIT).astype(jnp.float32)
        tail = jnp.where(lane == columns + slot, units, tail)
        sample = sample_ref[slot].astype(jnp.float32)
        tail = jnp.where(lane == columns + slots + slot, sample, tail)
    head = wide_ref[:, :last].astype(jnp.bfloat16)
    tail = tail.astype(jnp.bfloat16)
    for copy in range(copies):
        out_ref[copy, :, :last] = head
        out_ref[copy, :, last:] = tail
    for copy in range(proj_out_ref.shape[0]):
        proj_out_ref[copy] = proj_ref[...]


def payload_copies(image_patches, image_sample, w, copies, w_out, out_copies):
    rows, columns = w.shape
    lanes = -(-(columns + 2 * image_patches.shape[0]) // 128) * 128
    return pl.pallas_call(
        payload_kernel,
        in_specs=[pl.BlockSpec(memory_space=pltpu.SMEM)] * 2 + in_vmem(2),
        out_specs=in_vmem(2),
        out_shape=[
            jax.ShapeDtypeStruct((copies, rows, lanes), jnp.bfloat16),
            jax.ShapeDtypeStruct((out_copies, *w_out.shape), jnp.bfloat16),
        ],
        scratch_shapes=[pltpu.VMEM((rows, lanes), jnp.float32)],
        compiler_params=pltpu.CompilerParams(vmem_limit_bytes=8 << 20),
        name="payload_copies",
    )(in_hbm(image_patches), in_hbm(image_sample), in_hbm(w), in_hbm(w_out))


def normalize_kernel(x_ref, gain_ref, out_ref):
    x = x_ref[...].astype(jnp.float32)
    scale = lax.rsqrt(jnp.mean(x * x, axis=-1, keepdims=True) + epsilon)
    out_ref[...] = (x * scale * gain_ref[...]).astype(jnp.bfloat16).T


def normalize_rows(x, gain):
    return pl.pallas_call(
        normalize_kernel,
        in_specs=in_vmem(2),
        out_specs=pl.BlockSpec(memory_space=pltpu.VMEM),
        out_shape=jax.ShapeDtypeStruct((x.shape[1], x.shape[0]), jnp.bfloat16),
        compiler_params=pltpu.CompilerParams(vmem_limit_bytes=16 << 20),
        name="normalize_rows",
    )(x, gain)


def attention_kernel(
    normed_ref, w_ref, key_ref, query_ref, out_ref, qkv_ref, context_ref, *, head_width
):
    step = pl.program_id(0)
    chunk, width = w_ref.shape
    chunks = 3 * width // chunk

    @pl.when(step < chunks)
    def _():
        qkv_ref[pl.ds(pl.multiple_of(step * chunk, chunk), chunk), :] = jnp.dot(
            w_ref[...], normed_ref[...], preferred_element_type=jnp.float32
        ).astype(jnp.bfloat16)

    @pl.when(step >= chunks)
    def _():
        unit = step - chunks
        patches = pl.ds(pl.multiple_of(unit * UNIT, UNIT), UNIT)
        query_id = query_ref[pl.ds(unit, 1), :]
        key_id = jnp.broadcast_to(key_ref[pl.ds(unit, 1), :], (UNIT, UNIT)).T
        allowed = key_id == query_id
        heads = range(width // head_width)

        def rows(part, head):
            first = part * width + head * head_width
            return qkv_ref[first : first + head_width, patches]

        scores = [
            lax.dot_general(
                rows(1, head), rows(0, head), (((0,), (0,)), ((), ())), preferred_element_type=jnp.float32
            )
            for head in heads
        ]
        scores = [jnp.where(allowed, score, -1e30) for score in scores]
        highest = [jnp.max(score, axis=0, keepdims=True) for score in scores]
        factor = 1.0 / (math.sqrt(head_width) * math.log(2.0))
        weights = [jnp.exp2((score - top) * factor) for score, top in zip(scores, highest)]
        totals = [jnp.sum(weight, axis=0, keepdims=True) for weight in weights]
        weights = [
            (weight * jnp.where(query_id >= 0, 1.0 / total, 0.0)).astype(jnp.bfloat16)
            for weight, total in zip(weights, totals)
        ]
        for head, weight in zip(heads, weights):
            context_ref[head * head_width : (head + 1) * head_width, :] = jnp.dot(
                rows(2, head), weight, preferred_element_type=jnp.float32
            ).astype(jnp.bfloat16)
        out_ref[...] = context_ref[...].T


def attention(w, normed, key_id, query_id):
    width, count = normed.shape
    chunk = 3 * width // 4
    units = count // UNIT
    whole = lambda *shape: pl.BlockSpec(shape, lambda n: (0,) * len(shape))
    return pl.pallas_call(
        lambda *refs: attention_kernel(*refs, head_width=width // HEADS),
        grid=(4 + units,),
        in_specs=[
            whole(width, count),
            pl.BlockSpec((chunk, width), lambda n: (jnp.minimum(n, 3), 0)),
            whole(units, UNIT),
            whole(units, UNIT),
        ],
        out_specs=pl.BlockSpec((UNIT, width), lambda n: (jnp.maximum(n - 4, 0), 0)),
        out_shape=jax.ShapeDtypeStruct((count, width), jnp.bfloat16),
        scratch_shapes=[
            pltpu.VMEM((3 * width, count), jnp.bfloat16),
            pltpu.VMEM((width, UNIT), jnp.bfloat16),
        ],
        compiler_params=pltpu.CompilerParams(
            dimension_semantics=("arbitrary",), vmem_limit_bytes=32 << 20
        ),
        name="attention",
    )(in_hbm(normed), in_hbm(w), key_id, query_id)


def merge_kernel(
    core_ref, context_ref, w_own_ref, w_other_ref, x_ref, gain_ref, out_ref, hidden_ref, merged_ref, held_ref, formed_ref, sem, sems
):
    core = core_ref[0]
    count, width = context_ref.shape
    half = width // 2
    load = pltpu.make_async_copy(w_other_ref, held_ref, sem)
    load.start()
    hidden_ref[core] = jnp.dot(
        context_ref[...], w_own_ref[...], preferred_element_type=jnp.float32
    )
    load.wait()
    hidden_ref[1 - core] = jnp.dot(
        context_ref[...], held_ref[...], preferred_element_type=jnp.float32
    )
    low = x_ref[:, :half].astype(jnp.float32) + hidden_ref[0]
    high = x_ref[:, half:].astype(jnp.float32) + hidden_ref[1]
    square = jnp.sum(low * low, axis=-1, keepdims=True) + jnp.sum(
        high * high, axis=-1, keepdims=True
    )
    scale = lax.rsqrt(square * (1.0 / width) + epsilon)
    merged_ref[:, :half] = (low * scale * gain_ref[:, :half]).astype(jnp.bfloat16)
    merged_ref[:, half:] = (high * scale * gain_ref[:, half:]).astype(jnp.bfloat16)
    tokens = out_ref.shape[0] * out_ref.shape[1]
    units = count // UNIT
    to_row = lax.broadcasted_iota(jnp.int32, (tokens, count), 0)
    from_row = lax.broadcasted_iota(jnp.int32, (tokens, count), 1)
    stores = []
    first_row = (to_row % units) * UNIT + (to_row // units) * 4
    for member in range(4):
        choice = (from_row == first_row + member).astype(jnp.bfloat16)
        part = jnp.dot(choice, merged_ref[...], preferred_element_type=jnp.float32)
        columns = slice(member * width, (member + 1) * width)
        formed_ref[:, :, columns] = part.reshape(-1, units, width).astype(jnp.bfloat16)
        stores.append(
            pltpu.make_async_copy(
                formed_ref.at[:, :, columns], out_ref.at[:, :, columns], sems.at[member]
            )
        )
        stores[-1].start()
    for store in stores:
        store.wait()


def merge_tokens(core, context, w_own, w_other, x, gain):
    count, width = x.shape
    return pl.pallas_call(
        merge_kernel,
        in_specs=[pl.BlockSpec(memory_space=pltpu.SMEM)]
        + in_vmem(2)
        + [pl.BlockSpec(memory_space=pltpu.HBM)]
        + in_vmem(2),
        out_specs=pl.BlockSpec(memory_space=pltpu.HBM),
        out_shape=pltpu.HBM((UNIT // 4, count // UNIT, 4 * width), jnp.bfloat16),
        scratch_shapes=[
            pltpu.VMEM((2, count, width // 2), jnp.float32),
            pltpu.VMEM((count, width), jnp.bfloat16),
            pltpu.VMEM(w_other.shape, jnp.bfloat16),
            pltpu.VMEM((UNIT // 4, count // UNIT, 4 * width), jnp.bfloat16),
            pltpu.SemaphoreType.DMA,
            pltpu.SemaphoreType.DMA((4,)),
        ],
        compiler_params=pltpu.CompilerParams(vmem_limit_bytes=28 << 20),
        name="merge_tokens",
    )(core, context, w_own, in_hbm(w_other), x, gain)


def destination_rows(units, samples):
    slots = units.shape[1]
    samples = samples.reshape(-1)
    flat = units.reshape(-1)
    order = jnp.arange(flat.shape[0], dtype=jnp.int32)
    ahead = (samples[:, None] < samples[None, :]) | (
        (samples[:, None] == samples[None, :]) & (order[:, None] < order[None, :])
    )
    starts = jnp.sum(jnp.where(ahead, flat[:, None], 0), axis=0).reshape(units.shape)
    slot = jnp.arange(slots, dtype=jnp.int32)
    offsets = jnp.sum(jnp.where(slot[:, None] < slot[None, :], units[:, :, None], 0), axis=1)
    unit = slot[None, None, :]
    inside = (unit >= offsets[:, :, None]) & (unit < (offsets + units)[:, :, None])
    row = jnp.sum(jnp.where(inside, (starts - offsets)[:, :, None] + unit, 0), axis=1)
    return jnp.where(jnp.any(inside, axis=1), row, -1)


def body(patches, attn_gain, w_qkv, w_out, merge_gain, window_ids, image_patches, image_sample):
    patch_count, width = patches.shape
    token_count = patch_count // 4
    group_size = lax.axis_size("tensor")
    core = (lax.axis_index("pipe") % 2).astype(jnp.int32).reshape(1)

    half = width // 2
    slots = image_patches.shape[0]
    row_count, qkv_part = w_qkv.shape

    together = lax.optimization_barrier
    payload, out_copies = payload_copies(
        image_patches, image_sample, w_qkv, group_size, w_out, lax.axis_size("pipe")
    )
    rows = lax.all_to_all(payload, "tensor", 0, 0, tiled=True)
    slab = rows[:, :, :qkv_part].reshape(width, qkv_part).T
    w_all = lax.all_gather(slab, "pipe", axis=0, tiled=True)

    slab, out_copies, patches = together((slab, out_copies, patches))
    blocks = lax.all_to_all(out_copies, "pipe", 0, 0, tiled=True)
    normed = normalize_rows(patches, attn_gain[None, :])
    live = jnp.arange(patch_count, dtype=jnp.int32) < jnp.sum(image_patches)
    key_id = jnp.where(live, window_ids, -1).reshape(patch_count // UNIT, UNIT)
    query_id = jnp.where(live, window_ids, -2).reshape(patch_count // UNIT, UNIT)
    info = rows[:, 0, qkv_part : qkv_part + 2 * slots].astype(jnp.int32)
    merge_row = merge_gain[None, :]
    blocks, normed, key_id, query_id, info, merge_row = together(
        (blocks, normed, key_id, query_id, info, merge_row)
    )
    out_rows = jnp.moveaxis(blocks, 0, 1).reshape(row_count, 2, half)
    out_rows = lax.dynamic_index_in_dim(out_rows, core[0], axis=1, keepdims=False)
    out_own = copy_for_each(out_rows, "tensor").reshape(width, half)
    out_other = partner_copy(out_own)
    context = attention(w_all, normed, key_id, query_id)
    tokens = merge_tokens(core, context, out_own, out_other, patches, merge_row)
    tokens, info = together((tokens, info))
    dest_rows = destination_rows(info[:, :slots], info[:, slots:])
    received = lax.all_to_all(tokens, "tensor", split_axis=0, concat_axis=0, tiled=True)
    placement = (
        jnp.arange(token_count, dtype=jnp.int32)[:, None] == dest_rows.reshape(1, token_count)
    ).astype(jnp.bfloat16)
    placed = jnp.dot(
        placement, received.reshape(token_count, 4 * width), preferred_element_type=jnp.float32
    )
    return placed.astype(jnp.bfloat16).reshape(1, token_count, 1, 4 * width)


def solution(mesh):
    return jax.shard_map(
        body,
        mesh=mesh,
        in_specs=(
            P(("pipe", "tensor"), None),
            P(),
            P("tensor", "pipe"),
            P("tensor", "pipe"),
            P(),
            P(("pipe", "tensor")),
            P(("pipe", "tensor")),
            P(("pipe", "tensor")),
        ),
        out_specs=P("pipe", None, "tensor", None),
        check_vma=False,
    )
```
